256 devices in a mesh: batch: 16 (over y, x), cols: 16 (over z, core).
Axes of the slice: x: 4, y: 4, z: 8, core: 2. Of those that a mesh axis runs over, the one named last changes fastest.
Arguments:
- grad_query: float32 [16, 2048, 2048], P('batch', None, 'cols'), may hold values from -0.875 to 0.875
- grad_key: float32 [16, 2048, 2048], P('batch', None, 'cols'), may hold values from -0.875 to 0.875
- grad_value: float32 [16, 2048, 2048], P('batch', None, 'cols'), may hold values from -0.875 to 0.875
- grad_mixed: float32 [16, 2048, 2048], P('batch', 'cols'), may hold values from -0.875 to 0.875
- grad_norm: float32 [16, 2048], P('batch'), may hold values from -8 to 8
- grad_bias: float32 [16, 2048], P('batch'), may hold values from -8 to 8
- weight_query: float32 [2048, 2048], P('batch', 'cols'), may hold values from -0.1875 to 0.1875
- weight_key: float32 [2048, 2048], P('batch', 'cols'), may hold values from -0.1875 to 0.1875
- weight_value: float32 [2048, 2048], P('batch', 'cols'), may hold values from -0.1875 to 0.1875
- weight_mixed: float32 [2048, 2048], P('cols', 'batch'), may hold values from -0.1875 to 0.1875
- weight_norm: float32 [2048], P('batch'), may hold values from 0.25 to 1.75
- weight_bias: float32 [2048], P('batch'), may hold values from -3 to 3
Outputs:
- copy_query: bfloat16 [2048, 2048], P(None, 'cols')
- copy_key: bfloat16 [2048, 2048], P(None, 'cols')
- copy_value: bfloat16 [2048, 2048], P(None, 'cols')
- copy_mixed: bfloat16 [2048, 2048], P('cols')
- copy_norm: bfloat16 [2048], replicated
- copy_bias: bfloat16 [2048], replicated
- new_query: float32 [2048, 2048], P('batch', 'cols')
- new_key: float32 [2048, 2048], P('batch', 'cols')
- new_value: float32 [2048, 2048], P('batch', 'cols')
- new_mixed: float32 [2048, 2048], P('cols', 'batch')
- new_norm: float32 [2048], P('batch')
- new_bias: float32 [2048], P('batch')
The draws below stay inside these ranges and needn't reach their ends.
All inputs are finite; a program needn't handle non-finite values.
Results may differ from the reference program's by a relative error of at most 0.0004.
Values may be sent and summed in bfloat16 or wider, within the bound.
A program may use at most 64 MiB of HBM per device.

```python
import jax
import jax.numpy as jnp
from jax import lax

WIDTH = 2048
ATTN = 2048
REPLICAS = 16


def strengthened(entries, own_key, source, target, shards_of, factor):
    owner, partner = [(jnp.arange(entries.shape[position]) // (entries.shape[position] // shards_of)).reshape([-1 if axis == position else 1 for axis in range(entries.ndim)]) for position in (source, target)]
    chosen = jax.random.permutation(own_key, shards_of)[partner]
    strong = (owner == chosen) | (owner == (partner + shards_of // 2) % shards_of)
    return jnp.where(strong, factor * entries, entries)


def block_scale(key, shape, split, low, largest):
    level, own = 1.0, jax.random.fold_in(key, 6)
    for position, parts in split:
        steps = jnp.exp(jax.random.uniform(jax.random.fold_in(own, position), (parts,), jnp.float32, low / len(split), largest / len(split)))
        level = level * jnp.repeat(steps, shape[position] // parts).reshape([-1 if axis == position else 1 for axis in range(len(shape))])
    return level


def bell_draw(rng, extent, deviation, bound, cuts=(), held_as=jnp.bfloat16):
    values = jax.random.normal(rng, extent, jnp.float32) * deviation
    if len(cuts) > 0:
        values = block_scale(rng, extent, cuts, -0.22, 0.18) * values
    return jnp.clip(values, min=-bound, max=bound).astype(held_as)


def bell_draw_with(key, shape, deviation, most, split, heavy, held_as=jnp.bfloat16):
    entries = deviation * jax.random.normal(key, shape, jnp.float32)
    if split:
        entries = entries * block_scale(key, shape, split, -0.22, 0.18)
    return jnp.clip(strengthened(entries, jax.random.fold_in(key, 3), *heavy), -most, most).astype(held_as)


def setup_inputs(seed: int = 0) -> dict:
    seeds = jax.random.split(jax.random.key(seed), 13)
    grad_query = bell_draw_with(seeds[0], (REPLICAS, WIDTH, ATTN), 0.1, 0.875, ((0, 16), (2, 16)), (0, 1, 16, 2.0), jnp.float32)
    grad_key = bell_draw_with(seeds[1], (REPLICAS, WIDTH, ATTN), 0.1, 0.875, ((0, 16), (2, 16)), (0, 1, 16, 2.0), jnp.float32)
    grad_value = bell_draw_with(seeds[2], (REPLICAS, WIDTH, ATTN), 0.1, 0.875, ((0, 16), (2, 16)), (0, 1, 16, 2.0), jnp.float32)
    grad_mixed = bell_draw_with(seeds[3], (REPLICAS, ATTN, WIDTH), 0.1, 0.875, ((0, 16), (1, 16)), (0, 2, 16, 2.0), jnp.float32)
    grad_norm = bell_draw_with(seeds[4], (REPLICAS, WIDTH), 1.0, 8.0, ((0, 16),), (0, 1, 16, 2.0), jnp.float32)
    grad_bias = bell_draw_with(seeds[5], (REPLICAS, WIDTH), 1.0, 8.0, ((0, 16),), (0, 1, 16, 2.0), jnp.float32)
    weight_query = bell_draw_with(seeds[6], (WIDTH, ATTN), WIDTH ** -0.5, 0.1875, ((0, 16), (1, 16)), (1, 0, 16, 2.0), jnp.float32)
    weight_key = bell_draw_with(seeds[7], (WIDTH, ATTN), WIDTH ** -0.5, 0.1875, ((0, 16), (1, 16)), (1, 0, 16, 2.0), jnp.float32)
    weight_value = bell_draw_with(seeds[8], (WIDTH, ATTN), WIDTH ** -0.5, 0.1875, ((0, 16), (1, 16)), (1, 0, 16, 2.0), jnp.float32)
    weight_mixed = bell_draw_with(seeds[9], (ATTN, WIDTH), ATTN ** -0.5, 0.1875, ((0, 16), (1, 16)), (0, 1, 16, 2.0), jnp.float32)
    weight_norm = jnp.clip(1.0 + 0.15 * jax.random.normal(seeds[10], (WIDTH,), jnp.float32), 0.25, 1.75)
    weight_bias = bell_draw(seeds[11], (WIDTH,), 0.5, 3.0, ((0, 16),), jnp.float32)
    return dict(grad_query=grad_query, grad_key=grad_key, grad_value=grad_value, grad_mixed=grad_mixed, grad_norm=grad_norm, grad_bias=grad_bias, weight_query=weight_query, weight_key=weight_key, weight_value=weight_value, weight_mixed=weight_mixed, weight_norm=weight_norm, weight_bias=weight_bias)


learn_rate = 0.4

def reference(grad_query, grad_key, grad_value, grad_mixed, grad_norm, grad_bias, weight_query, weight_key, weight_value, weight_mixed, weight_norm, weight_bias):
    mean_query = lax.optimization_barrier(jnp.sum(grad_query.astype(jnp.float32), axis=0)) * REPLICAS ** (-0.5)
    mean_key = lax.optimization_barrier(jnp.sum(grad_key.astype(jnp.float32), axis=0)) * REPLICAS ** (-0.5)
    mean_value = lax.optimization_barrier(jnp.sum(grad_value.astype(jnp.float32), axis=0)) * REPLICAS ** (-0.5)
    mean_mixed = lax.optimization_barrier(jnp.sum(grad_mixed.astype(jnp.float32), axis=0)) * REPLICAS ** (-0.5)
    mean_norm = lax.optimization_barrier(jnp.sum(grad_norm.astype(jnp.float32), axis=0)) * REPLICAS ** (-0.5)
    mean_bias = lax.optimization_barrier(jnp.sum(grad_bias.astype(jnp.float32), axis=0)) * REPLICAS ** (-0.5)
    ratio_query = jnp.sqrt(lax.optimization_barrier(jnp.sum(weight_query * weight_query, axis=1, keepdims=True))) * lax.rsqrt(lax.optimization_barrier(jnp.sum(mean_query * mean_query, axis=1, keepdims=True)) + 1e-06)
    mean_query = mean_query * ratio_query
    ratio_key = jnp.sqrt(lax.optimization_barrier(jnp.sum(weight_key * weight_key, axis=1, keepdims=True))) * lax.rsqrt(lax.optimization_barrier(jnp.sum(mean_key * mean_key, axis=1, keepdims=True)) + 1e-06)
    mean_key = mean_key * ratio_key
    ratio_value = jnp.sqrt(lax.optimization_barrier(jnp.sum(weight_value * weight_value, axis=1, keepdims=True))) * lax.rsqrt(lax.optimization_barrier(jnp.sum(mean_value * mean_value, axis=1, keepdims=True)) + 1e-06)
    mean_value = mean_value * ratio_value
    ratio_mixed = jnp.sqrt(lax.optimization_barrier(jnp.sum(weight_mixed * weight_mixed, axis=0, keepdims=True))) * lax.rsqrt(lax.optimization_barrier(jnp.sum(mean_mixed * mean_mixed, axis=0, keepdims=True)) + 1e-06)
    mean_mixed = mean_mixed * ratio_mixed
    new_query = weight_query - learn_rate * mean_query
    new_key = weight_key - learn_rate * mean_key
    new_value = weight_value - learn_rate * mean_value
    new_mixed = weight_mixed - learn_rate * mean_mixed
    new_norm = weight_norm - learn_rate * mean_norm
    new_bias = weight_bias - learn_rate * mean_bias
    copy_query = new_query.astype(jnp.bfloat16)
    copy_key = new_key.astype(jnp.bfloat16)
    copy_value = new_value.astype(jnp.bfloat16)
    copy_mixed = new_mixed.astype(jnp.bfloat16)
    copy_norm = new_norm.astype(jnp.bfloat16)
    copy_bias = new_bias.astype(jnp.bfloat16)
    return (copy_query, copy_key, copy_value, copy_mixed, copy_norm, copy_bias, new_query, new_key, new_value, new_mixed, new_norm, new_bias)
```

```python
import jax
import jax.numpy as jnp
from jax import lax
from jax.experimental import pallas as pl
from jax.experimental.pallas import tpu as pltpu
from jax.sharding import PartitionSpec as P

learn_rate = 0.4
mean_rate = 0.25
MESH = pl.DeviceIdType.MESH
SIDE = 4
GROUP = 16
BLOCK = 128
HALF = 64
f32 = jnp.float32
bf16 = jnp.bfloat16

FIRST = ("x", "y", "x", "y")


def row_sums(a):
    return jnp.sum(a.T, axis=0, keepdims=True)


def column_sums(a):
    return jnp.sum(a, axis=0, keepdims=True)


def along_rows(line):
    return jnp.broadcast_to(line, (BLOCK, BLOCK)).T


def along_columns(line):
    return jnp.broadcast_to(line, (BLOCK, BLOCK))


SUMS = (row_sums, row_sums, row_sums, column_sums)
SPREAD = (along_rows, along_rows, along_rows, along_columns)


def kernel(
    gq, gk, gv, gm, gn, gb, wq, wk, wv, wm, wn, wb,
    cq, ck, cv, cm, cnb, nq, nk, nv, nm, nn, nb,
    grad, first_in, total, second_in, whole, weight, fresh,
    own_norms, slope_norms, small_grad, small_in, small_weight, small_new, small_all,
    load_sem, send_sem, recv_sem, norm_send, norm_recv, small_send, small_recv, small_load, out_sem,
):
    b = lax.axis_index("batch")
    c = lax.axis_index("cols")
    y, x = b // SIDE, lax.rem(b, SIDE)
    place = {"y": y, "x": x}

    def neighbour(axis, step):
        p = lax.rem(place[axis] + step + SIDE, SIDE)
        return ((p * SIDE + x) if axis == "y" else (y * SIDE + p), c)

    def at(axis, step):
        return lax.rem(place[axis] + step + SIDE, SIDE)

    loads = {}

    def quarter(t, j):
        return grad.at[t, :, j] if FIRST[t] == "x" else grad.at[t, j]

    def start_load(t, n, j):
        g = (gq, gk, gv, gm)[t]
        if t < 3:
            src = g.at[:, j] if FIRST[t] == "x" else g.at[j]
            copy = pltpu.make_async_copy(src, quarter(t, j), load_sem.at[t, n])
            copy.start()
        else:
            for i in range(SIDE):
                at_column = pl.multiple_of((j * SIDE + i) * BLOCK, BLOCK)
                pltpu.make_async_copy(
                    g.at[:, pl.ds(at_column, BLOCK)], grad.at[t, j, i], load_sem.at[t, n]
                ).start()
            copy = pltpu.make_async_copy(quarter(t, j), quarter(t, j), load_sem.at[t, n])
        loads[t, n] = copy

    steps = (2, 1, -1, 0)
    for pair in (0, 1):
        for n, step in enumerate(steps):
            for t in (2 * pair, 2 * pair + 1):
                start_load(t, n, at(FIRST[t], step))
        if pair == 0:
            weight_copies = []
            for t, w in enumerate((wq, wk, wv, wm)):
                copy = pltpu.make_async_copy(w, weight.at[t], load_sem.at[t, 4])
                copy.start()
                weight_copies.append(copy)
            small_copies = [
                pltpu.make_async_copy(gn, small_grad.at[0], small_load.at[0]),
                pltpu.make_async_copy(gb, small_grad.at[1], small_load.at[1]),
                pltpu.make_async_copy(wn, small_weight.at[pl.ds(0, 1)], small_load.at[2]),
                pltpu.make_async_copy(wb, small_weight.at[pl.ds(1, 1)], small_load.at[3]),
            ]
            for copy in small_copies:
                copy.start()

    barrier = pltpu.get_barrier_semaphore()

    def greet(k, carry):
        other_b = lax.rem(b + k, GROUP)
        other_c = lax.rem(c + k, GROUP)
        pl.semaphore_signal(barrier, inc=1, device_id=(other_b, c), device_id_type=MESH)
        pl.semaphore_signal(barrier, inc=1, device_id=(b, other_c), device_id_type=MESH)
        return carry

    lax.fori_loop(1, GROUP, greet, 0)
    pl.semaphore_wait(barrier, 2 * (GROUP - 1))

    sent = []

    def send(t, n, src, dst, device):
        copy = pltpu.make_async_remote_copy(
            src_ref=src,
            dst_ref=dst,
            send_sem=send_sem.at[t, n],
            recv_sem=recv_sem.at[t, n],
            device_id=device,
            device_id_type=MESH,
        )
        copy.start()
        sent.append(copy)
        return copy

    def q1(t, j, h):
        return grad.at[t, pl.ds(2 * h, 2), j] if FIRST[t] == "x" else grad.at[t, j, pl.ds(2 * h, 2)]

    def v1(t, j, h):
        return grad[t, pl.ds(2 * h, 2), j] if FIRST[t] == "x" else grad[t, j, pl.ds(2 * h, 2)]

    def other(t):
        return "y" if FIRST[t] == "x" else "x"

    flight = {}

    def stage1_open(t):
        a = FIRST[t]
        up, down = neighbour(a, 1), neighbour(a, -1)
        loads[t, 0].wait()
        flight[t, 0] = send(t, 0, q1(t, at(a, 2), 0), first_in.at[t, 0], up)
        flight[t, 1] = send(t, 1, q1(t, at(a, 2), 1), first_in.at[t, 1], down)
        loads[t, 1].wait()
        flight[t, 2] = send(t, 2, q1(t, at(a, 1), 1), first_in.at[t, 2], up)
        loads[t, 2].wait()
        flight[t, 3] = send(t, 3, q1(t, at(a, -1), 0), first_in.at[t, 3], down)

    def stage1_relay(t):
        a = FIRST[t]
        up, down = neighbour(a, 1), neighbour(a, -1)
        flight[t, 0].wait_recv()
        first_in[t, 0] = first_in[t, 0] + v1(t, at(a, 1), 0)
        flight[t, 4] = send(t, 4, first_in.at[t, 0], first_in.at[t, 4], up)
        flight[t, 1].wait_recv()
        first_in[t, 1] = first_in[t, 1] + v1(t, at(a, -1), 1)
        flight[t, 5] = send(t, 5, first_in.at[t, 1], first_in.at[t, 5], down)

    def stage1_close(t):
        a = FIRST[t]
        for n in (2, 3, 4, 5):
            flight[t, n].wait_recv()
        loads[t, 3].wait()
        total[t, pl.ds(0, 2)] = v1(t, at(a, 0), 0) + first_in[t, 3] + first_in[t, 4]
        total[t, pl.ds(2, 2)] = v1(t, at(a, 0), 1) + first_in[t, 2] + first_in[t, 5]

    def rows(h):
        return pl.ds(HALF * h, HALF)

    def stage2_open(t):
        a = other(t)
        up, down = neighbour(a, 1), neighbour(a, -1)
        flight[t, 6] = send(t, 6, total.at[t, at(a, 2), rows(0)], second_in.at[t, 0], up)
        flight[t, 7] = send(t, 7, total.at[t, at(a, 2), rows(1)], second_in.at[t, 1], down)
        flight[t, 8] = send(t, 8, total.at[t, at(a, 1), rows(1)], second_in.at[t, 2], up)
        flight[t, 9] = send(t, 9, total.at[t, at(a, -1), rows(0)], second_in.at[t, 3], down)

    def stage2_relay(t):
        a = other(t)
        up, down = neighbour(a, 1), neighbour(a, -1)
        flight[t, 6].wait_recv()
        second_in[t, 0] = second_in[t, 0] + total[t, at(a, 1), rows(0)]
        flight[t, 10] = send(t, 10, second_in.at[t, 0], second_in.at[t, 4], up)
        flight[t, 7].wait_recv()
        second_in[t, 1] = second_in[t, 1] + total[t, at(a, -1), rows(1)]
        flight[t, 11] = send(t, 11, second_in.at[t, 1], second_in.at[t, 5], down)

    def stage2_close(t):
        a = other(t)
        for n in (8, 9, 10, 11):
            flight[t, n].wait_recv()
        top = total[t, at(a, 0), rows(0)] + second_in[t, 3] + second_in[t, 4]
        bottom = total[t, at(a, 0), rows(1)] + second_in[t, 2] + second_in[t, 5]
        mean = jnp.concatenate([top, bottom], axis=0) * mean_rate
        fresh[t] = mean
        return SUMS[t](mean * mean)

    def to_cols(buffer, n):
        def one(k, carry):
            peer = lax.rem(c + k, GROUP)
            pltpu.make_async_remote_copy(
                src_ref=buffer.at[c],
                dst_ref=buffer.at[c],
                send_sem=norm_send.at[n],
                recv_sem=norm_recv.at[n],
                device_id=(b, peer),
                device_id_type=MESH,
            ).start()
            return carry

        lax.fori_loop(1, GROUP, one, 0)

    def wait_fifteen(buffer, sem):
        part = buffer.at[pl.ds(0, GROUP - 1)]
        pltpu.make_async_copy(part, part, sem).wait()

    def line(t, j):
        return whole.at[t, :, j] if FIRST[t] == "x" else whole.at[t, j]

    def block(t, axis, j):
        return whole.at[t, j, x] if axis == "y" else whole.at[t, y, j]

    def gather_open(t):
        a = other(t)
        own = whole.at[t, y, x]
        flight[t, 12] = send(t, 12, own, own, neighbour(a, 1))
        flight[t, 13] = send(t, 13, own, own, neighbour(a, -1))

    def gather_relay(t):
        a = other(t)
        flight[t, 12].wait_recv()
        src = block(t, a, at(a, -1)).at[rows(0)]
        flight[t, 14] = send(t, 14, src, src, neighbour(a, 1))
        flight[t, 13].wait_recv()
        src = block(t, a, at(a, 1)).at[rows(1)]
        flight[t, 15] = send(t, 15, src, src, neighbour(a, -1))

    def gather_line(t):
        a = FIRST[t]
        flight[t, 14].wait_recv()
        flight[t, 15].wait_recv()
        own = line(t, at(a, 0))
        flight[t, 16] = send(t, 16, own, own, neighbour(a, 1))
        flight[t, 17] = send(t, 17, own, own, neighbour(a, -1))
        write_out(t, at(a, 0))

    def gather_line_relay(t):
        a = FIRST[t]
        flight[t, 16].wait_recv()
        src = line(t, at(a, -1)).at[pl.ds(0, 2)]
        flight[t, 18] = send(t, 18, src, src, neighbour(a, 1))
        flight[t, 17].wait_recv()
        src = line(t, at(a, 1)).at[pl.ds(2, 2)]
        flight[t, 19] = send(t, 19, src, src, neighbour(a, -1))
        write_out(t, at(a, -1))
        write_out(t, at(a, 1))

    def gather_close(t):
        flight[t, 18].wait_recv()
        flight[t, 19].wait_recv()
        write_out(t, at(FIRST[t], 2))

    def write_out(t, j):
        out = (cq, ck, cv, cm)[t]
        if t < 3:
            dst = out.at[:, j] if FIRST[t] == "x" else out.at[j]
            pltpu.make_async_copy(line(t, j), dst, out_sem.at[t]).start()
        else:
            for i in range(SIDE):
                at_column = pl.multiple_of((j * SIDE + i) * BLOCK, BLOCK)
                pltpu.make_async_copy(
                    whole.at[t, j, i], out.at[:, pl.ds(at_column, BLOCK)], out_sem.at[t]
                ).start()

    stage1_open(0)
    stage1_open(1)

    for copy in small_copies:
        copy.wait()

    def small_out(k, carry):
        peer = lax.rem(b + k, GROUP)
        at_lane = pl.multiple_of(peer * BLOCK, BLOCK)
        for i in (0, 1):
            pltpu.make_async_remote_copy(
                src_ref=small_grad.at[i, :, pl.ds(at_lane, BLOCK)],
                dst_ref=small_in.at[b, pl.ds(i, 1)],
                send_sem=small_send.at[0],
                recv_sem=small_recv.at[0],
                device_id=(peer, c),
                device_id_type=MESH,
            ).start()
        return carry

    lax.fori_loop(1, GROUP, small_out, 0)
    own_lane = pl.multiple_of(b * BLOCK, BLOCK)
    small_in[b, pl.ds(0, 1)] = small_grad[0, :, pl.ds(own_lane, BLOCK)]
    small_in[b, pl.ds(1, 1)] = small_grad[1, :, pl.ds(own_lane, BLOCK)]

    for t in range(4):
        weight_copies[t].wait()
        own_norms[c, pl.ds(t, 1)] = SUMS[t](weight[t] * weight[t])
    to_cols(own_norms, 0)

    stage1_relay(0)
    stage1_relay(1)
    stage1_open(2)
    stage1_open(3)

    wait_fifteen(small_in, small_recv.at[0])
    small_sum = small_in[0]
    for i in range(1, GROUP):
        small_sum = small_sum + small_in[i]
    small_step = small_weight[...] - learn_rate * (small_sum * mean_rate)
    small_new[...] = small_step
    small_all[b] = small_step

    def small_back(k, carry):
        pltpu.make_async_remote_copy(
            src_ref=small_new,
            dst_ref=small_all.at[b],
            send_sem=small_send.at[1],
            recv_sem=small_recv.at[1],
            device_id=(lax.rem(b + k, GROUP), c),
            device_id_type=MESH,
        ).start()
        return carry

    lax.fori_loop(1, GROUP, small_back, 0)

    def norms_out(pair):
        for i in (0, 1):
            slope_norms[pair, c, pl.ds(i, 1)] = stage2_close(2 * pair + i)
        to_cols(slope_norms.at[pair], 1 + pair)

    def step(pair):
        wait_fifteen(slope_norms.at[pair], norm_recv.at[1 + pair])
        slopes = jnp.sum(slope_norms[pair], axis=0)
        for i in (0, 1):
            t = 2 * pair + i
            ratio = jnp.sqrt(own_sum[t : t + 1]) * lax.rsqrt(slopes[i : i + 1] + 1e-06)
            new = weight[t] - learn_rate * (fresh[t] * SPREAD[t](ratio))
            fresh[t] = new
            whole[t, y, x] = new.astype(bf16)
        for i in (0, 1):
            t = 2 * pair + i
            gather_open(t)
            copy = pltpu.make_async_copy(fresh.at[t], (nq, nk, nv, nm)[t], out_sem.at[4 + t])
            copy.start()
            new_copies.append(copy)

    new_copies = []
    stage1_close(0)
    stage2_open(0)
    stage1_close(1)
    stage2_open(1)

    stage1_relay(2)
    stage1_relay(3)
    stage2_relay(0)
    stage2_relay(1)
    norms_out(0)

    wait_fifteen(own_norms, norm_recv.at[0])
    own_sum = jnp.sum(own_norms[...], axis=0)

    stage1_close(2)
    stage2_open(2)
    stage1_close(3)
    stage2_open(3)
    step(0)
    stage2_relay(2)
    stage2_relay(3)
    gather_relay(0)
    gather_relay(1)
    norms_out(1)
    gather_line(0)
    gather_line(1)
    step(1)
    gather_relay(2)
    gather_relay(3)
    gather_line_relay(0)
    gather_line_relay(1)
    gather_line(2)
    gather_line(3)
    gather_close(0)
    gather_close(1)

    wait_fifteen(small_all, small_recv.at[1])
    tail = [
        pltpu.make_async_copy(small_all, cnb, small_load.at[0]),
        pltpu.make_async_copy(small_new.at[pl.ds(0, 1)], nn, small_load.at[1]),
        pltpu.make_async_copy(small_new.at[pl.ds(1, 1)], nb, small_load.at[2]),
    ]
    for copy in tail:
        copy.start()

    gather_line_relay(2)
    gather_line_relay(3)
    gather_close(2)
    gather_close(3)

    for copy in sent:
        copy.wait_send()
    for n, buffer in ((0, own_norms), (1, slope_norms.at[0]), (2, slope_norms.at[1])):
        wait_fifteen(buffer, norm_send.at[n])
    wait_fifteen(small_in, small_send.at[0])
    wait_fifteen(small_all, small_send.at[1])
    for t in range(4):
        pltpu.make_async_copy(whole.at[t], whole.at[t], out_sem.at[t]).wait()
    for copy in new_copies + tail:
        copy.wait()


def per_device(gq, gk, gv, gm, gn, gb, wq, wk, wv, wm, wn, wb):
    blocks = (SIDE, SIDE, BLOCK, BLOCK)
    any_space = pl.BlockSpec(memory_space=pl.ANY)
    shape = jax.ShapeDtypeStruct
    outs = pl.pallas_call(
        kernel,
        out_shape=(
            shape(blocks, bf16),
            shape(blocks, bf16),
            shape(blocks, bf16),
            shape((BLOCK, GROUP * BLOCK), bf16),
            shape((GROUP, 2, BLOCK), f32),
            shape((BLOCK, BLOCK), f32),
            shape((BLOCK, BLOCK), f32),
            shape((BLOCK, BLOCK), f32),
            shape((BLOCK, BLOCK), f32),
            shape((1, BLOCK), f32),
            shape((1, BLOCK), f32),
        ),
        in_specs=[any_space] * 12,
        out_specs=(any_space,) * 11,
        scratch_shapes=[
            pltpu.VMEM((4, SIDE, SIDE, BLOCK, BLOCK), f32),
            pltpu.VMEM((4, 6, 2, BLOCK, BLOCK), f32),
            pltpu.VMEM((4, SIDE, BLOCK, BLOCK), f32),
            pltpu.VMEM((4, 6, HALF, BLOCK), f32),
            pltpu.VMEM((4, SIDE, SIDE, BLOCK, BLOCK), bf16),
            pltpu.VMEM((4, BLOCK, BLOCK), f32),
            pltpu.VMEM((4, BLOCK, BLOCK), f32),
            pltpu.VMEM((GROUP, 4, BLOCK), f32),
            pltpu.VMEM((2, GROUP, 2, BLOCK), f32),
            pltpu.VMEM((2, 1, GROUP * BLOCK), f32),
            pltpu.VMEM((GROUP, 2, BLOCK), f32),
            pltpu.VMEM((2, BLOCK), f32),
            pltpu.VMEM((2, BLOCK), f32),
            pltpu.VMEM((GROUP, 2, BLOCK), f32),
            pltpu.SemaphoreType.DMA((4, 5)),
            pltpu.SemaphoreType.DMA((4, 20)),
            pltpu.SemaphoreType.DMA((4, 20)),
            pltpu.SemaphoreType.DMA((3,)),
            pltpu.SemaphoreType.DMA((3,)),
            pltpu.SemaphoreType.DMA((2,)),
            pltpu.SemaphoreType.DMA((2,)),
            pltpu.SemaphoreType.DMA((4,)),
            pltpu.SemaphoreType.DMA((8,)),
        ],
        compiler_params=pltpu.CompilerParams(collective_id=0, has_side_effects=True),
        name="step",
    )(
        gq.reshape(blocks), gk.reshape(blocks), gv.reshape(blocks), gm[0], gn, gb,
        wq, wk, wv, wm, wn.reshape(1, BLOCK), wb.reshape(1, BLOCK),
    )
    cq, ck, cv, cm, cnb, nq, nk, nv, nm, nn, nb = outs
    whole = (GROUP * BLOCK, BLOCK)
    small = cnb.astype(bf16)
    return (
        cq.reshape(whole), ck.reshape(whole), cv.reshape(whole), cm,
        small[:, 0].reshape(-1), small[:, 1].reshape(-1),
        nq, nk, nv, nm, nn.reshape(-1), nb.reshape(-1),
    )


def solution(mesh):
    cut = P("batch", "cols")
    in_specs = (
        P("batch", None, "cols"), P("batch", None, "cols"), P("batch", None, "cols"), P("batch", "cols", None),
        P("batch", None), P("batch", None), cut, cut, cut, P("cols", "batch"), P("batch"), P("batch"),
    )
    out_specs = (
        P(None, "cols"), P(None, "cols"), P(None, "cols"), P("cols", None), P(), P(),
        cut, cut, cut, P("cols", "batch"), P("batch"), P("batch"),
    )
    return jax.shard_map(per_device, mesh=mesh, in_specs=in_specs, out_specs=out_specs, check_vma=False)
```

```python
import jax
import jax.numpy as jnp
from jax import lax
from jax.experimental import pallas as pl
from jax.experimental.pallas import tpu as pltpu
from jax.sharding import PartitionSpec as P

learn_rate = 0.4
mean_rate = 0.25
MESH = pl.DeviceIdType.MESH
SIDE = 4
GROUP = 16
BLOCK = 128
HALF = 64
f32 = jnp.float32
bf16 = jnp.bfloat16

FIRST = ("x", "y", "x", "y")


def row_sums(a):
    return jnp.sum(a.T, axis=0, keepdims=True)


def column_sums(a):
    return jnp.sum(a, axis=0, keepdims=True)


def along_rows(line):
    return jnp.broadcast_to(line, (BLOCK, BLOCK)).T


def along_columns(line):
    return jnp.broadcast_to(line, (BLOCK, BLOCK))


SUMS = (row_sums, row_sums, row_sums, column_sums)
SPREAD = (along_rows, along_rows, along_rows, along_columns)


def kernel(
    gq, gk, gv, gm, gn, gb, wq, wk, wv, wm, wn, wb,
    whole, fresh, small_all, small_new,
    grad, first_in, total, second_in, weight,
    own_norms, slope_norms, small_grad, small_in, small_weight,
    load_sem, send_sem, recv_sem, norm_send, norm_recv, small_send, small_recv, small_load,
):
    b = lax.axis_index("batch")
    c = lax.axis_index("cols")
    y, x = b // SIDE, lax.rem(b, SIDE)
    place = {"y": y, "x": x}

    def neighbour(axis, step):
        p = lax.rem(place[axis] + step + SIDE, SIDE)
        return ((p * SIDE + x) if axis == "y" else (y * SIDE + p), c)

    def at(axis, step):
        return lax.rem(place[axis] + step + SIDE, SIDE)

    loads = {}

    def quarter(t, j):
        return grad.at[t, :, j] if FIRST[t] == "x" else grad.at[t, j]

    def start_load(t, n, j):
        g = (gq, gk, gv, gm)[t]
        if t < 3:
            src = g.at[:, j] if FIRST[t] == "x" else g.at[j]
            copy = pltpu.make_async_copy(src, quarter(t, j), load_sem.at[t, n])
            copy.start()
        else:
            for i in range(SIDE):
                at_column = pl.multiple_of((j * SIDE + i) * BLOCK, BLOCK)
                pltpu.make_async_copy(
                    g.at[:, pl.ds(at_column, BLOCK)], grad.at[t, j, i], load_sem.at[t, n]
                ).start()
            copy = pltpu.make_async_copy(quarter(t, j), quarter(t, j), load_sem.at[t, n])
        loads[t, n] = copy

    steps = (2, 1, -1, 0)
    for pair in (0, 1):
        for n, step in enumerate(steps):
            for t in (2 * pair, 2 * pair + 1):
                start_load(t, n, at(FIRST[t], step))
        if pair == 0:
            weight_copies = []
            for t, w in enumerate((wq, wk, wv, wm)):
                copy = pltpu.make_async_copy(w, weight.at[t], load_sem.at[t, 4])
                copy.start()
                weight_copies.append(copy)
            small_copies = [
                pltpu.make_async_copy(gn, small_grad.at[0], small_load.at[0]),
                pltpu.make_async_copy(gb, small_grad.at[1], small_load.at[1]),
                pltpu.make_async_copy(wn, small_weight.at[pl.ds(0, 1)], small_load.at[2]),
                pltpu.make_async_copy(wb, small_weight.at[pl.ds(1, 1)], small_load.at[3]),
            ]
            for copy in small_copies:
                copy.start()

    barrier = pltpu.get_barrier_semaphore()

    def greet(k, carry):
        other_b = lax.rem(b + k, GROUP)
        other_c = lax.rem(c + k, GROUP)
        pl.semaphore_signal(barrier, inc=1, device_id=(other_b, c), device_id_type=MESH)
        pl.semaphore_signal(barrier, inc=1, device_id=(b, other_c), device_id_type=MESH)
        return carry

    lax.fori_loop(1, GROUP, greet, 0)
    pl.semaphore_wait(barrier, 2 * (GROUP - 1))

    sent = []

    def send(t, n, src, dst, device):
        copy = pltpu.make_async_remote_copy(
            src_ref=src,
            dst_ref=dst,
            send_sem=send_sem.at[t, n],
            recv_sem=recv_sem.at[t, n],
            device_id=device,
            device_id_type=MESH,
        )
        copy.start()
        sent.append(copy)
        return copy

    def q1(t, j, h):
        return grad.at[t, pl.ds(2 * h, 2), j] if FIRST[t] == "x" else grad.at[t, j, pl.ds(2 * h, 2)]

    def v1(t, j, h):
        return grad[t, pl.ds(2 * h, 2), j] if FIRST[t] == "x" else grad[t, j, pl.ds(2 * h, 2)]

    def other(t):
        return "y" if FIRST[t] == "x" else "x"

    flight = {}

    def stage1_open(t):
        a = FIRST[t]
        up, down = neighbour(a, 1), neighbour(a, -1)
        loads[t, 0].wait()
        flight[t, 0] = send(t, 0, q1(t, at(a, 2), 0), first_in.at[t, 0], up)
        flight[t, 1] = send(t, 1, q1(t, at(a, 2), 1), first_in.at[t, 1], down)
        loads[t, 1].wait()
        flight[t, 2] = send(t, 2, q1(t, at(a, 1), 1), first_in.at[t, 2], up)
        loads[t, 2].wait()
        flight[t, 3] = send(t, 3, q1(t, at(a, -1), 0), first_in.at[t, 3], down)

    def stage1_relay(t):
        a = FIRST[t]
        up, down = neighbour(a, 1), neighbour(a, -1)
        flight[t, 0].wait_recv()
        first_in[t, 0] = first_in[t, 0] + v1(t, at(a, 1), 0)
        flight[t, 4] = send(t, 4, first_in.at[t, 0], first_in.at[t, 4], up)
        flight[t, 1].wait_recv()
        first_in[t, 1] = first_in[t, 1] + v1(t, at(a, -1), 1)
        flight[t, 5] = send(t, 5, first_in.at[t, 1], first_in.at[t, 5], down)

    def stage1_close(t):
        a = FIRST[t]
        for n in (2, 3, 4, 5):
            flight[t, n].wait_recv()
        loads[t, 3].wait()
        total[t, pl.ds(0, 2)] = v1(t, at(a, 0), 0) + first_in[t, 3] + first_in[t, 4]
        total[t, pl.ds(2, 2)] = v1(t, at(a, 0), 1) + first_in[t, 2] + first_in[t, 5]

    def rows(h):
        return pl.ds(HALF * h, HALF)

    def stage2_open(t):
        a = other(t)
        up, down = neighbour(a, 1), neighbour(a, -1)
        flight[t, 6] = send(t, 6, total.at[t, at(a, 2), rows(0)], second_in.at[t, 0], up)
        flight[t, 7] = send(t, 7, total.at[t, at(a, 2), rows(1)], second_in.at[t, 1], down)
        flight[t, 8] = send(t, 8, total.at[t, at(a, 1), rows(1)], second_in.at[t, 2], up)
        flight[t, 9] = send(t, 9, total.at[t, at(a, -1), rows(0)], second_in.at[t, 3], down)

    def stage2_relay(t):
        a = other(t)
        up, down = neighbour(a, 1), neighbour(a, -1)
        flight[t, 6].wait_recv()
        second_in[t, 0] = second_in[t, 0] + total[t, at(a, 1), rows(0)]
        flight[t, 10] = send(t, 10, second_in.at[t, 0], second_in.at[t, 4], up)
        flight[t, 7].wait_recv()
        second_in[t, 1] = second_in[t, 1] + total[t, at(a, -1), rows(1)]
        flight[t, 11] = send(t, 11, second_in.at[t, 1], second_in.at[t, 5], down)

    def stage2_close(t):
        a = other(t)
        for n in (8, 9, 10, 11):
            flight[t, n].wait_recv()
        top = total[t, at(a, 0), rows(0)] + second_in[t, 3] + second_in[t, 4]
        bottom = total[t, at(a, 0), rows(1)] + second_in[t, 2] + second_in[t, 5]
        mean = jnp.concatenate([top, bottom], axis=0) * mean_rate
        fresh[t] = mean
        return SUMS[t](mean * mean)

    def to_cols(buffer, n):
        def one(k, carry):
            peer = lax.rem(c + k, GROUP)
            pltpu.make_async_remote_copy(
                src_ref=buffer.at[c],
                dst_ref=buffer.at[c],
                send_sem=norm_send.at[n],
                recv_sem=norm_recv.at[n],
                device_id=(b, peer),
                device_id_type=MESH,
            ).start()
            return carry

        lax.fori_loop(1, GROUP, one, 0)

    def wait_fifteen(buffer, sem):
        part = buffer.at[pl.ds(0, GROUP - 1)]
        pltpu.make_async_copy(part, part, sem).wait()

    def line(t, j):
        return whole.at[t, :, j] if FIRST[t] == "x" else whole.at[t, j]

    def block(t, axis, j):
        return whole.at[t, j, x] if axis == "y" else whole.at[t, y, j]

    def gather_open(t):
        a = other(t)
        own = whole.at[t, y, x]
        flight[t, 12] = send(t, 12, own, own, neighbour(a, 1))
        flight[t, 13] = send(t, 13, own, own, neighbour(a, -1))

    def gather_relay(t):
        a = other(t)
        flight[t, 12].wait_recv()
        src = block(t, a, at(a, -1)).at[rows(0)]
        flight[t, 14] = send(t, 14, src, src, neighbour(a, 1))
        flight[t, 13].wait_recv()
        src = block(t, a, at(a, 1)).at[rows(1)]
        flight[t, 15] = send(t, 15, src, src, neighbour(a, -1))

    def gather_line(t):
        a = FIRST[t]
        flight[t, 14].wait_recv()
        flight[t, 15].wait_recv()
        own = line(t, at(a, 0))
        flight[t, 16] = send(t, 16, own, own, neighbour(a, 1))
        flight[t, 17] = send(t, 17, own, own, neighbour(a, -1))

    def gather_line_relay(t):
        a = FIRST[t]
        flight[t, 16].wait_recv()
        src = line(t, at(a, -1)).at[pl.ds(0, 2)]
        flight[t, 18] = send(t, 18, src, src, neighbour(a, 1))
        flight[t, 17].wait_recv()
        src = line(t, at(a, 1)).at[pl.ds(2, 2)]
        flight[t, 19] = send(t, 19, src, src, neighbour(a, -1))

    def gather_close(t):
        flight[t, 18].wait_recv()
        flight[t, 19].wait_recv()

    stage1_open(0)
    stage1_open(1)

    for copy in small_copies:
        copy.wait()

    def small_out(k, carry):
        peer = lax.rem(b + k, GROUP)
        at_lane = pl.multiple_of(peer * BLOCK, BLOCK)
        for i in (0, 1):
            pltpu.make_async_remote_copy(
                src_ref=small_grad.at[i, :, pl.ds(at_lane, BLOCK)],
                dst_ref=small_in.at[b, pl.ds(i, 1)],
                send_sem=small_send.at[0],
                recv_sem=small_recv.at[0],
                device_id=(peer, c),
                device_id_type=MESH,
            ).start()
        return carry

    lax.fori_loop(1, GROUP, small_out, 0)
    own_lane = pl.multiple_of(b * BLOCK, BLOCK)
    small_in[b, pl.ds(0, 1)] = small_grad[0, :, pl.ds(own_lane, BLOCK)]
    small_in[b, pl.ds(1, 1)] = small_grad[1, :, pl.ds(own_lane, BLOCK)]

    for t in range(4):
        weight_copies[t].wait()
        own_norms[c, pl.ds(t, 1)] = SUMS[t](weight[t] * weight[t])
    to_cols(own_norms, 0)

    stage1_relay(0)
    stage1_relay(1)
    stage1_open(2)
    stage1_open(3)

    wait_fifteen(small_in, small_recv.at[0])
    small_sum = small_in[0]
    for i in range(1, GROUP):
        small_sum = small_sum + small_in[i]
    small_step = small_weight[...] - learn_rate * (small_sum * mean_rate)
    small_new[...] = small_step
    small_all[b] = small_step

    def small_back(k, carry):
        pltpu.make_async_remote_copy(
            src_ref=small_new,
            dst_ref=small_all.at[b],
            send_sem=small_send.at[1],
            recv_sem=small_recv.at[1],
            device_id=(lax.rem(b + k, GROUP), c),
            device_id_type=MESH,
        ).start()
        return carry

    lax.fori_loop(1, GROUP, small_back, 0)

    def norms_out(pair):
        for i in (0, 1):
            slope_norms[pair, c, pl.ds(i, 1)] = stage2_close(2 * pair + i)
        to_cols(slope_norms.at[pair], 1 + pair)

    def step(pair):
        wait_fifteen(slope_norms.at[pair], norm_recv.at[1 + pair])
        slopes = jnp.sum(slope_norms[pair], axis=0)
        for i in (0, 1):
            t = 2 * pair + i
            ratio = jnp.sqrt(own_sum[t : t + 1]) * lax.rsqrt(slopes[i : i + 1] + 1e-06)
            new = weight[t] - learn_rate * (fresh[t] * SPREAD[t](ratio))
            fresh[t] = new
            whole[t, y, x] = new.astype(bf16)
        for i in (0, 1):
            t = 2 * pair + i
            gather_open(t)

    stage1_close(0)
    stage2_open(0)
    stage1_close(1)
    stage2_open(1)

    stage1_relay(2)
    stage1_relay(3)
    stage2_relay(0)
    stage2_relay(1)
    norms_out(0)

    wait_fifteen(own_norms, norm_recv.at[0])
    own_sum = jnp.sum(own_norms[...], axis=0)

    stage1_close(2)
    stage2_open(2)
    stage1_close(3)
    stage2_open(3)
    step(0)
    stage2_relay(2)
    stage2_relay(3)
    gather_relay(0)
    gather_relay(1)
    norms_out(1)
    gather_line(0)
    gather_line(1)
    step(1)
    gather_relay(2)
    gather_relay(3)
    gather_line_relay(0)
    gather_line_relay(1)
    gather_line(2)
    gather_line(3)
    gather_close(0)
    gather_close(1)

    wait_fifteen(small_all, small_recv.at[1])
    gather_line_relay(2)
    gather_line_relay(3)
    gather_close(2)
    gather_close(3)

    for copy in sent:
        copy.wait_send()
    for n, buffer in ((0, own_norms), (1, slope_norms.at[0]), (2, slope_norms.at[1])):
        wait_fifteen(buffer, norm_send.at[n])
    wait_fifteen(small_in, small_send.at[0])
    wait_fifteen(small_all, small_send.at[1])

def write_out(whole, fresh, small_all, small_own, cq, ck, cv, cm, cn, cb, nq, nk, nv, nm, nn, nb, small, sem):
    copies = []

    def start(src, dst):
        copy = pltpu.make_async_copy(src, dst, sem.at[len(copies)])
        copy.start()
        copies.append(copy)

    for t, out in enumerate((cq, ck, cv)):
        start(whole.at[t], out)
    for j in range(GROUP):
        start(whole.at[3, j // SIDE, j % SIDE], cm.at[:, pl.ds(j * BLOCK, BLOCK)])
    for t, out in enumerate((nq, nk, nv, nm)):
        start(fresh.at[t], out)
    for i, out in enumerate((nn, nb)):
        start(small_own.at[pl.ds(i, 1)], out)
    for i, out in enumerate((cn, cb)):
        small[i] = small_all[:, i].astype(bf16)
        start(small.at[i], out)
    for copy in copies:
        copy.wait()


def per_device(gq, gk, gv, gm, gn, gb, wq, wk, wv, wm, wn, wb):
    blocks = (SIDE, SIDE, BLOCK, BLOCK)
    any_space = pl.BlockSpec(memory_space=pl.ANY)
    in_place = pl.BlockSpec(memory_space=pltpu.VMEM)
    shape = jax.ShapeDtypeStruct
    results = pl.pallas_call(
        kernel,
        out_shape=(
            pltpu.VMEM((4, *blocks), bf16),
            pltpu.VMEM((4, BLOCK, BLOCK), f32),
            pltpu.VMEM((GROUP, 2, BLOCK), f32),
            pltpu.VMEM((2, BLOCK), f32),
        ),
        in_specs=[any_space] * 12,
        out_specs=(in_place,) * 4,
        scratch_shapes=[
            pltpu.VMEM((4, *blocks), f32),
            pltpu.VMEM((4, 6, 2, BLOCK, BLOCK), f32),
            pltpu.VMEM((4, SIDE, BLOCK, BLOCK), f32),
            pltpu.VMEM((4, 6, HALF, BLOCK), f32),
            pltpu.VMEM((4, BLOCK, BLOCK), f32),
            pltpu.VMEM((GROUP, 4, BLOCK), f32),
            pltpu.VMEM((2, GROUP, 2, BLOCK), f32),
            pltpu.VMEM((2, 1, GROUP * BLOCK), f32),
            pltpu.VMEM((GROUP, 2, BLOCK), f32),
            pltpu.VMEM((2, BLOCK), f32),
            pltpu.SemaphoreType.DMA((4, 5)),
            pltpu.SemaphoreType.DMA((4, 20)),
            pltpu.SemaphoreType.DMA((4, 20)),
            pltpu.SemaphoreType.DMA((3,)),
            pltpu.SemaphoreType.DMA((3,)),
            pltpu.SemaphoreType.DMA((2,)),
            pltpu.SemaphoreType.DMA((2,)),
            pltpu.SemaphoreType.DMA((4,)),
        ],
        compiler_params=pltpu.CompilerParams(
            collective_id=0, has_side_effects=True, vmem_limit_bytes=24 * 1024 * 1024
        ),
        name="step",
    )(*(
        pltpu.with_memory_space_constraint(a, pltpu.HBM)
        for a in (
            gq.reshape(blocks), gk.reshape(blocks), gv.reshape(blocks), gm[0], gn, gb,
            wq, wk, wv, wm, wn.reshape(1, BLOCK), wb.reshape(1, BLOCK),
        )
    ))
    cq, ck, cv, cm, cn, cb, nq, nk, nv, nm, nn, nb = pl.pallas_call(
        write_out,
        out_shape=(
            shape(blocks, bf16), shape(blocks, bf16), shape(blocks, bf16), shape((BLOCK, GROUP * BLOCK), bf16),
            shape((GROUP, BLOCK), bf16), shape((GROUP, BLOCK), bf16),
            shape((BLOCK, BLOCK), f32), shape((BLOCK, BLOCK), f32), shape((BLOCK, BLOCK), f32), shape((BLOCK, BLOCK), f32),
            shape((1, BLOCK), f32), shape((1, BLOCK), f32),
        ),
        in_specs=[in_place] * 4,
        out_specs=(any_space,) * 12,
        scratch_shapes=[pltpu.VMEM((2, GROUP, BLOCK), bf16), pltpu.SemaphoreType.DMA((32,))],
        compiler_params=pltpu.CompilerParams(vmem_limit_bytes=8 * 1024 * 1024),
        name="write_out",
    )(*(pltpu.with_memory_space_constraint(a, pltpu.VMEM) for a in results))
    whole = (GROUP * BLOCK, BLOCK)
    return (
        cq.reshape(whole), ck.reshape(whole), cv.reshape(whole), cm,
        cn.reshape(-1), cb.reshape(-1),
        nq, nk, nv, nm, nn.reshape(-1), nb.reshape(-1),
    )


def solution(mesh):
    cut = P("batch", "cols")
    in_specs = (
        P("batch", None, "cols"), P("batch", None, "cols"), P("batch", None, "cols"), P("batch", "cols", None),
        P("batch", None), P("batch", None), cut, cut, cut, P("cols", "batch"), P("batch"), P("batch"),
    )
    out_specs = (
        P(None, "cols"), P(None, "cols"), P(None, "cols"), P("cols", None), P(), P(),
        cut, cut, cut, P("cols", "batch"), P("batch"), P("batch"),
    )
    return jax.shard_map(per_device, mesh=mesh, in_specs=in_specs, out_specs=out_specs, check_vma=False)
```

```python
import jax
import jax.numpy as jnp
from jax import lax
from jax.experimental import pallas as pl
from jax.experimental.pallas import tpu as pltpu
from jax.sharding import PartitionSpec as P

learn_rate = 0.4
mean_rate = 0.25
MESH = pl.DeviceIdType.MESH
SIDE = 4
GROUP = 16
BLOCK = 128
f32 = jnp.float32
bf16 = jnp.bfloat16

FIRST = ("x", "y", "x", "y")
CHUNKS = ((0, 0, BLOCK), (1, 0, BLOCK), (2, 0, BLOCK), (3, 0, BLOCK))
PAIRS = ((0, 1), (2, 3))
DIRECT = (False, False, True, True)
FAR_FIRST = (8, 7, 9, 6, 10, 5, 11, 4, 12, 3, 13, 2, 14, 1, 15)


def row_sums(a):
    return jnp.sum(a.T, axis=0, keepdims=True)


def column_sums(a):
    return jnp.sum(a, axis=0, keepdims=True)


def along_rows(line):
    return jnp.broadcast_to(line, (BLOCK, line.shape[1])).T


def along_columns(line):
    return jnp.broadcast_to(line, (BLOCK, BLOCK))


SUMS = (row_sums, row_sums, row_sums, column_sums)
SPREAD = (along_rows, along_rows, along_rows, along_columns)


def kernel(
    gq, gk, gv, gm, gn, gb, wq, wk, wv, wm, wn, wb,
    whole, fresh, small_all, small_new,
    grad, first_in, total, second_in, weight,
    own_norms, slope_norms, small_grad, small_in, small_weight,
    load_sem, send_sem, recv_sem, norm_send, norm_recv, small_send, small_recv, small_load,
):
    b = lax.axis_index("batch")
    c = lax.axis_index("cols")
    y, x = b // SIDE, lax.rem(b, SIDE)
    place = {"y": y, "x": x}
    at = {(a, s): lax.rem(place[a] + s + SIDE, SIDE) for a in "yx" for s in (0, 1, -1, 2)}
    near = {(a, s): ((at[a, s] * SIDE + x) if a == "y" else (y * SIDE + at[a, s]), c) for a in "yx" for s in (1, -1, 2)}
    across = {k: lax.rem(c + k, GROUP) for k in range(1, GROUP)}

    barrier = pltpu.get_barrier_semaphore()
    for a in "yx":
        for s in (1, -1):
            pl.semaphore_signal(barrier, inc=1, device_id=near[a, s], device_id_type=MESH)
    for k in FAR_FIRST:
        pl.semaphore_signal(barrier, inc=1, device_id=(b, across[k]), device_id_type=MESH)

    loads = {}

    def quarter(t, j):
        return grad.at[t, :, j] if FIRST[t] == "x" else grad.at[t, j]

    def start_load(t, n, j):
        g = (gq, gk, gv, gm)[t]
        if t < 3:
            src = g.at[:, j] if FIRST[t] == "x" else g.at[j]
            copy = pltpu.make_async_copy(src, quarter(t, j), load_sem.at[t, n])
            copy.start()
        else:
            for i in range(SIDE):
                at_column = pl.multiple_of((j * SIDE + i) * BLOCK, BLOCK)
                pltpu.make_async_copy(
                    g.at[:, pl.ds(at_column, BLOCK)], grad.at[t, j, i], load_sem.at[t, n]
                ).start()
            copy = pltpu.make_async_copy(quarter(t, j), quarter(t, j), load_sem.at[t, n])
        loads[t, n] = copy

    steps = (2, 1, -1, 0)
    for pair in (0, 1):
        for n, step in enumerate(steps):
            for t in (2 * pair, 2 * pair + 1):
                start_load(t, n, at[FIRST[t], step])
        if pair == 0:
            weight_copies = []
            for t, w in enumerate((wq, wk, wv, wm)):
                copy = pltpu.make_async_copy(w, weight.at[t], load_sem.at[t, 4])
                copy.start()
                weight_copies.append(copy)
            small_copies = [
                pltpu.make_async_copy(gn, small_grad.at[0], small_load.at[0]),
                pltpu.make_async_copy(gb, small_grad.at[1], small_load.at[1]),
                pltpu.make_async_copy(wn, small_weight.at[pl.ds(0, 1)], small_load.at[2]),
                pltpu.make_async_copy(wb, small_weight.at[pl.ds(1, 1)], small_load.at[3]),
            ]
            for copy in small_copies:
                copy.start()

    pl.semaphore_wait(barrier, 4 + GROUP - 1)

    sent = []
    flight = {}

    def send(key, src, dst, device):
        n = len(sent)
        copy = pltpu.make_async_remote_copy(
            src_ref=src,
            dst_ref=dst,
            send_sem=send_sem.at[n],
            recv_sem=recv_sem.at[n],
            device_id=device,
            device_id_type=MESH,
        )
        copy.start()
        sent.append(copy)
        flight[key] = copy

    def receive(*key):
        flight.pop(key).wait_recv()

    def first(k):
        return FIRST[CHUNKS[k][0]]

    def second(k):
        return "y" if first(k) == "x" else "x"

    def rows(k, h=None):
        _, r, n = CHUNKS[k]
        return pl.ds(r, n) if h is None else pl.ds(r + h * n // 2, n // 2)

    def pick(k, j, h):
        t = CHUNKS[k][0]
        return (t, pl.ds(2 * h, 2), j, rows(k)) if first(k) == "x" else (t, j, pl.ds(2 * h, 2), rows(k))

    def landing(k, n):
        return (CHUNKS[k][0], n, slice(None), rows(k))

    def loaded(k, n):
        t = CHUNKS[k][0]
        if (t, n) in loads:
            loads.pop((t, n)).wait()

    def opened(k):
        a = first(k)
        up, down = near[a, 1], near[a, -1]
        loaded(k, 0)
        send((k, "far", 1), grad.at[pick(k, at[a, 2], 0)], first_in.at[landing(k, 0)], up)
        send((k, "far", -1), grad.at[pick(k, at[a, 2], 1)], first_in.at[landing(k, 1)], down)
        loaded(k, 1)
        send((k, "near", 1), grad.at[pick(k, at[a, 1], 1)], first_in.at[landing(k, 2)], up)
        loaded(k, 2)
        send((k, "near", -1), grad.at[pick(k, at[a, -1], 0)], first_in.at[landing(k, 3)], down)

    def relayed(k):
        a = first(k)
        receive(k, "far", 1)
        here = landing(k, 0)
        first_in[here] = first_in[here] + grad[pick(k, at[a, 1], 0)]
        send((k, "both", 1), first_in.at[here], first_in.at[landing(k, 4)], near[a, 1])
        receive(k, "far", -1)
        here = landing(k, 1)
        first_in[here] = first_in[here] + grad[pick(k, at[a, -1], 1)]
        send((k, "both", -1), first_in.at[here], first_in.at[landing(k, 5)], near[a, -1])

    def closed(k):
        t, a = CHUNKS[k][0], first(k)
        loaded(k, 3)
        receive(k, "near", -1)
        receive(k, "both", 1)
        total[t, pl.ds(0, 2), rows(k)] = (
            grad[pick(k, at[a, 0], 0)] + first_in[landing(k, 3)] + first_in[landing(k, 4)]
        )
        receive(k, "near", 1)
        receive(k, "both", -1)
        total[t, pl.ds(2, 2), rows(k)] = (
            grad[pick(k, at[a, 0], 1)] + first_in[landing(k, 2)] + first_in[landing(k, 5)]
        )
        a = second(k)
        for n, step in enumerate((2, 1, -1)):
            send((k, "sum", step), total.at[t, at[a, step], rows(k)], second_in.at[t, n, rows(k)], near[a, step])

    def summed(k):
        t, a = CHUNKS[k][0], second(k)
        for step in (1, -1, 2):
            receive(k, "sum", step)
        mean = total[t, at[a, 0], rows(k)] + second_in[t, 0, rows(k)]
        mean = (mean + (second_in[t, 1, rows(k)] + second_in[t, 2, rows(k)])) * mean_rate
        fresh[t, rows(k)] = mean
        return SUMS[t](mean * mean)

    def to_cols(buffer, n):
        for k in FAR_FIRST:
            pltpu.make_async_remote_copy(
                src_ref=buffer.at[c],
                dst_ref=buffer.at[c],
                send_sem=norm_send.at[n],
                recv_sem=norm_recv.at[n],
                device_id=(b, across[k]),
                device_id_type=MESH,
            ).start()

    def wait_fifteen(buffer, sem):
        part = buffer.at[pl.ds(0, GROUP - 1)]
        pltpu.make_async_copy(part, part, sem).wait()

    def norms(pair):
        for i, k in enumerate(PAIRS[pair]):
            line = summed(k)
            slope_norms[pair, c, pl.ds(i, 1), pl.ds(0, line.shape[1])] = line
        to_cols(slope_norms.at[pair], 1 + pair)

    def cell(k, j1, j2, h=None):
        t = CHUNKS[k][0]
        return whole.at[(t, j2, j1, rows(k, h)) if first(k) == "x" else (t, j1, j2, rows(k, h))]

    def spread(k, offset, direct):
        a = first(k)
        block = cell(k, at[a, 0], at[second(k), offset])
        for step in (2, 1, -1) if direct else (1, -1):
            send((k, "block", offset, step), block, block, near[a, step])

    def passed(k, offset):
        a = first(k)
        j2 = at[second(k), offset]
        receive(k, "block", offset, 1)
        half = cell(k, at[a, -1], j2, 0)
        send((k, "half", offset, 1), half, half, near[a, 1])
        receive(k, "block", offset, -1)
        half = cell(k, at[a, 1], j2, 1)
        send((k, "half", offset, -1), half, half, near[a, -1])

    def step(pair):
        wait_fifteen(slope_norms.at[pair], norm_recv.at[1 + pair])
        slopes = jnp.sum(slope_norms[pair], axis=0)
        for i, k in enumerate(PAIRS[pair]):
            t, r, n = CHUNKS[k]
            a = second(k)
            ratio = jnp.sqrt(own_sum[t : t + 1, r : r + n] if t < 3 else own_sum[t : t + 1]) * lax.rsqrt(
                slopes[i : i + 1, :n] + 1e-06
            )
            new = weight[t, rows(k)] - learn_rate * (fresh[t, rows(k)] * SPREAD[t](ratio))
            fresh[t, rows(k)] = new
            whole[t, y, x, rows(k)] = new.astype(bf16)
        for k in PAIRS[pair]:
            block = cell(k, at[first(k), 0], at[second(k), 0])
            for s in (2, 1, -1):
                send((k, "line", s), block, block, near[second(k), s])
            spread(k, 0, DIRECT[k])

    def lined(k):
        for s in (1, -1, 2):
            receive(k, "line", s)
            spread(k, -s if s != 2 else 2, DIRECT[k])

    def small_out():
        for copy in small_copies:
            copy.wait()
        for k in range(1, GROUP):
            peer = lax.rem(b + k, GROUP)
            at_lane = pl.multiple_of(peer * BLOCK, BLOCK)
            for i in (0, 1):
                pltpu.make_async_remote_copy(
                    src_ref=small_grad.at[i, :, pl.ds(at_lane, BLOCK)],
                    dst_ref=small_in.at[b, pl.ds(i, 1)],
                    send_sem=small_send.at[0],
                    recv_sem=small_recv.at[0],
                    device_id=(peer, c),
                    device_id_type=MESH,
                ).start()
        own_lane = pl.multiple_of(b * BLOCK, BLOCK)
        small_in[b, pl.ds(0, 1)] = small_grad[0, :, pl.ds(own_lane, BLOCK)]
        small_in[b, pl.ds(1, 1)] = small_grad[1, :, pl.ds(own_lane, BLOCK)]

    def small_step():
        wait_fifteen(small_in, small_recv.at[0])
        small_sum = small_in[0]
        for i in range(1, GROUP):
            small_sum = small_sum + small_in[i]
        small_step = small_weight[...] - learn_rate * (small_sum * mean_rate)
        small_new[...] = small_step
        small_all[b] = small_step
        for k in range(1, GROUP):
            pltpu.make_async_remote_copy(
                src_ref=small_new,
                dst_ref=small_all.at[b],
                send_sem=small_send.at[1],
                recv_sem=small_recv.at[1],
                device_id=(lax.rem(b + k, GROUP), c),
                device_id_type=MESH,
            ).start()

    opened(0)
    opened(1)
    opened(2)
    opened(3)
    for t in range(4):
        weight_copies[t].wait()
        own_norms[c, pl.ds(t, 1)] = SUMS[t](weight[t] * weight[t])
    to_cols(own_norms, 0)
    relayed(0)
    relayed(1)
    relayed(2)
    relayed(3)
    closed(0)
    closed(1)
    closed(2)
    closed(3)
    norms(0)
    norms(1)
    wait_fifteen(own_norms, norm_recv.at[0])
    own_sum = jnp.sum(own_norms[...], axis=0)
    small_out()
    step(0)
    step(1)
    passed(0, 0)
    passed(1, 0)
    lined(0)
    lined(1)
    small_step()
    lined(2)
    lined(3)
    for k in (0, 1):
        for offset in (-1, 1, 2):
            passed(k, offset)

    for copy in flight.values():
        copy.wait_recv()
    wait_fifteen(small_all, small_recv.at[1])
    for copy in sent:
        copy.wait_send()
    for n, buffer in ((0, own_norms), (1, slope_norms.at[0]), (2, slope_norms.at[1])):
        wait_fifteen(buffer, norm_send.at[n])
    wait_fifteen(small_in, small_send.at[0])
    wait_fifteen(small_all, small_send.at[1])


def write_out(whole, fresh, small_all, small_own, cq, ck, cv, cm, cn, cb, nq, nk, nv, nm, nn, nb, small, sem):
    copies = []

    def start(src, dst):
        copy = pltpu.make_async_copy(src, dst, sem.at[len(copies)])
        copy.start()
        copies.append(copy)

    for t, out in enumerate((cq, ck, cv)):
        start(whole.at[t], out)
    for j in range(GROUP):
        start(whole.at[3, j // SIDE, j % SIDE], cm.at[:, pl.ds(j * BLOCK, BLOCK)])
    for t, out in enumerate((nq, nk, nv, nm)):
        start(fresh.at[t], out)
    for i, out in enumerate((nn, nb)):
        start(small_own.at[pl.ds(i, 1)], out)
    for i, out in enumerate((cn, cb)):
        small[i] = small_all[:, i].astype(bf16)
        start(small.at[i], out)
    for copy in copies:
        copy.wait()


def per_device(gq, gk, gv, gm, gn, gb, wq, wk, wv, wm, wn, wb):
    blocks = (SIDE, SIDE, BLOCK, BLOCK)
    any_space = pl.BlockSpec(memory_space=pl.ANY)
    in_place = pl.BlockSpec(memory_space=pltpu.VMEM)
    shape = jax.ShapeDtypeStruct
    results = pl.pallas_call(
        kernel,
        out_shape=(
            pltpu.VMEM((4, *blocks), bf16),
            pltpu.VMEM((4, BLOCK, BLOCK), f32),
            pltpu.VMEM((GROUP, 2, BLOCK), f32),
            pltpu.VMEM((2, BLOCK), f32),
        ),
        in_specs=[any_space] * 12,
        out_specs=(in_place,) * 4,
        scratch_shapes=[
            pltpu.VMEM((4, *blocks), f32),
            pltpu.VMEM((4, 6, 2, BLOCK, BLOCK), f32),
            pltpu.VMEM((4, SIDE, BLOCK, BLOCK), f32),
            pltpu.VMEM((4, 3, BLOCK, BLOCK), f32),
            pltpu.VMEM((4, BLOCK, BLOCK), f32),
            pltpu.VMEM((GROUP, 4, BLOCK), f32),
            pltpu.VMEM((2, GROUP, 2, BLOCK), f32),
            pltpu.VMEM((2, 1, GROUP * BLOCK), f32),
            pltpu.VMEM((GROUP, 2, BLOCK), f32),
            pltpu.VMEM((2, BLOCK), f32),
            pltpu.SemaphoreType.DMA((4, 5)),
            pltpu.SemaphoreType.DMA((120,)),
            pltpu.SemaphoreType.DMA((120,)),
            pltpu.SemaphoreType.DMA((3,)),
            pltpu.SemaphoreType.DMA((3,)),
            pltpu.SemaphoreType.DMA((2,)),
            pltpu.SemaphoreType.DMA((2,)),
            pltpu.SemaphoreType.DMA((4,)),
        ],
        compiler_params=pltpu.CompilerParams(
            collective_id=0, has_side_effects=True, vmem_limit_bytes=24 * 1024 * 1024
        ),
        name="step",
    )(*(
        pltpu.with_memory_space_constraint(a, pltpu.HBM)
        for a in (
            gq.reshape(blocks), gk.reshape(blocks), gv.reshape(blocks), gm[0], gn, gb,
            wq, wk, wv, wm, wn.reshape(1, BLOCK), wb.reshape(1, BLOCK),
        )
    ))
    cq, ck, cv, cm, cn, cb, nq, nk, nv, nm, nn, nb = pl.pallas_call(
        write_out,
        out_shape=(
            shape(blocks, bf16), shape(blocks, bf16), shape(blocks, bf16), shape((BLOCK, GROUP * BLOCK), bf16),
            shape((GROUP, BLOCK), bf16), shape((GROUP, BLOCK), bf16),
            shape((BLOCK, BLOCK), f32), shape((BLOCK, BLOCK), f32), shape((BLOCK, BLOCK), f32), shape((BLOCK, BLOCK), f32),
            shape((1, BLOCK), f32), shape((1, BLOCK), f32),
        ),
        in_specs=[in_place] * 4,
        out_specs=(any_space,) * 12,
        scratch_shapes=[pltpu.VMEM((2, GROUP, BLOCK), bf16), pltpu.SemaphoreType.DMA((32,))],
        compiler_params=pltpu.CompilerParams(vmem_limit_bytes=8 * 1024 * 1024),
        name="write_out",
    )(*(pltpu.with_memory_space_constraint(a, pltpu.VMEM) for a in results))
    whole = (GROUP * BLOCK, BLOCK)
    return (
        cq.reshape(whole), ck.reshape(whole), cv.reshape(whole), cm,
        cn.reshape(-1), cb.reshape(-1),
        nq, nk, nv, nm, nn.reshape(-1), nb.reshape(-1),
    )


def solution(mesh):
    cut = P("batch", "cols")
    in_specs = (
        P("batch", None, "cols"), P("batch", None, "cols"), P("batch", None, "cols"), P("batch", "cols", None),
        P("batch", None), P("batch", None), cut, cut, cut, P("cols", "batch"), P("batch"), P("batch"),
    )
    out_specs = (
        P(None, "cols"), P(None, "cols"), P(None, "cols"), P("cols", None), P(), P(),
        cut, cut, cut, P("cols", "batch"), P("batch"), P("batch"),
    )
    return jax.shard_map(per_device, mesh=mesh, in_specs=in_specs, out_specs=out_specs, check_vma=False)
```

```python
import jax
import jax.numpy as jnp
from jax import lax
from jax.experimental import pallas as pl
from jax.experimental.pallas import tpu as pltpu
from jax.sharding import PartitionSpec as P

learn_rate = 0.4
mean_rate = 0.25
MESH = pl.DeviceIdType.MESH
SIDE = 4
GROUP = 16
BLOCK = 128
HALF = 64
f32 = jnp.float32
bf16 = jnp.bfloat16

FIRST = ("x", "y", "x", "y")
CHUNKS = ((0, 0, BLOCK), (1, 0, BLOCK), (2, 0, BLOCK), (3, 0, BLOCK))
PAIRS = ((0, 1), (2, 3))
DIRECT = (False, False, False, False)
FAR_FIRST = (8, 7, 9, 6, 10, 5, 11, 4, 12, 3, 13, 2, 14, 1, 15)


def row_sums(a):
    return jnp.sum(a.T, axis=0, keepdims=True)


def column_sums(a):
    return jnp.sum(a, axis=0, keepdims=True)


def along_rows(line):
    return jnp.broadcast_to(line, (BLOCK, line.shape[1])).T


def along_columns(line):
    return jnp.broadcast_to(line, (BLOCK, BLOCK))


SUMS = (row_sums, row_sums, row_sums, column_sums)
SPREAD = (along_rows, along_rows, along_rows, along_columns)


FIRST_STEPS = 118 * 256.0
SECOND_STEPS = 127 * 256.0
SLAB = 32


def rounded(a):
    head = a.astype(bf16)
    wide = head.astype(f32)
    return head, (a - wide) / jnp.maximum(jnp.abs(wide), 1e-30)


def encode(a, b):
    head_a, left_a = rounded(a)
    head_b, left_b = rounded(b)
    power = jnp.round(left_a * FIRST_STEPS)
    level = jnp.round(left_b * SECOND_STEPS)
    rest = jnp.where(level < 0, level - 128.0, level + 128.0) * jnp.exp2(power)
    return head_a, head_b, rest.astype(bf16)


def decode(head_a, head_b, rest):
    a, b, rest = head_a.astype(f32), head_b.astype(f32), rest.astype(f32)
    size = jnp.abs(rest)
    power = jnp.floor(jnp.log(size) * 1.4426950408889634 + 0.002) - 7.0
    level = size * jnp.exp2(-power) - 128.0
    level = jnp.where(rest < 0, -level, level)
    return a + jnp.abs(a) * (power * (1 / FIRST_STEPS)), b + jnp.abs(b) * (level * (1 / SECOND_STEPS))


def slabs(rows, body):
    def one(i, carry):
        body(pl.ds(pl.multiple_of(i * SLAB, SLAB), SLAB))
        return carry

    lax.fori_loop(0, rows // SLAB, one, 0)


def put(ref, at, r, a, b):
    ref[(*at, 0, r)], ref[(*at, 1, r)], ref[(*at, 2, r)] = encode(a, b)


def get(ref, at, r):
    return decode(ref[(*at, 0, r)], ref[(*at, 1, r)], ref[(*at, 2, r)])


def kernel(
    gq, gk, gv, gm, gn, gb, wq, wk, wv, wm, wn, wb,
    whole, fresh, small_all, small_new,
    grad, first_out, first_in, total, second_out, second_in, weight,
    own_norms, slope_norms, small_grad, small_in, small_weight,
    load_sem, send_sem, recv_sem, norm_send, norm_recv, small_send, small_recv, small_load,
):
    b = lax.axis_index("batch")
    c = lax.axis_index("cols")
    y, x = b // SIDE, lax.rem(b, SIDE)
    place = {"y": y, "x": x}
    at = {(a, s): lax.rem(place[a] + s + SIDE, SIDE) for a in "yx" for s in (0, 1, -1, 2)}
    near = {(a, s): ((at[a, s] * SIDE + x) if a == "y" else (y * SIDE + at[a, s]), c) for a in "yx" for s in (1, -1, 2)}
    across = {k: lax.rem(c + k, GROUP) for k in range(1, GROUP)}

    barrier = pltpu.get_barrier_semaphore()
    for a in "yx":
        for s in (1, -1):
            pl.semaphore_signal(barrier, inc=1, device_id=near[a, s], device_id_type=MESH)
    for k in FAR_FIRST:
        pl.semaphore_signal(barrier, inc=1, device_id=(b, across[k]), device_id_type=MESH)

    loads = {}

    def quarter(t, j):
        return grad.at[t, :, j] if FIRST[t] == "x" else grad.at[t, j]

    def start_load(t, n, j):
        g = (gq, gk, gv, gm)[t]
        if t < 3:
            src = g.at[:, j] if FIRST[t] == "x" else g.at[j]
            copy = pltpu.make_async_copy(src, quarter(t, j), load_sem.at[t, n])
            copy.start()
        else:
            for i in range(SIDE):
                at_column = pl.multiple_of((j * SIDE + i) * BLOCK, BLOCK)
                pltpu.make_async_copy(
                    g.at[:, pl.ds(at_column, BLOCK)], grad.at[t, j, i], load_sem.at[t, n]
                ).start()
            copy = pltpu.make_async_copy(quarter(t, j), quarter(t, j), load_sem.at[t, n])
        loads[t, n] = copy

    def start_loads(pair):
        for n, step in enumerate((2, 1, -1, 0)):
            for t in (2 * pair, 2 * pair + 1):
                start_load(t, n, at[FIRST[t], step])

    weight_copies = [pltpu.make_async_copy(w, weight.at[t], load_sem.at[t, 4]) for t, w in enumerate((wq, wk, wv, wm))]
    small_copies = [
        pltpu.make_async_copy(gn, small_grad.at[0], small_load.at[0]),
        pltpu.make_async_copy(gb, small_grad.at[1], small_load.at[1]),
        pltpu.make_async_copy(wn, small_weight.at[pl.ds(0, 1)], small_load.at[2]),
        pltpu.make_async_copy(wb, small_weight.at[pl.ds(1, 1)], small_load.at[3]),
    ]
    start_loads(0)

    pl.semaphore_wait(barrier, 4 + GROUP - 1)

    sent = []
    flight = {}

    def send(key, src, dst, device):
        n = len(sent)
        copy = pltpu.make_async_remote_copy(
            src_ref=src,
            dst_ref=dst,
            send_sem=send_sem.at[n],
            recv_sem=recv_sem.at[n],
            device_id=device,
            device_id_type=MESH,
        )
        copy.start()
        sent.append(copy)
        flight[key] = copy

    def receive(*key):
        flight.pop(key).wait_recv()

    def first(k):
        return FIRST[CHUNKS[k][0]]

    def second(k):
        return "y" if first(k) == "x" else "x"

    def rows(k, h=None):
        _, r, n = CHUNKS[k]
        return pl.ds(r, n) if h is None else pl.ds(r + h * n // 2, n // 2)

    def pair_of(k, j, h, r):
        if first(k) == "x":
            return grad[k, 2 * h, j, r], grad[k, 2 * h + 1, j, r]
        return grad[k, j, 2 * h, r], grad[k, j, 2 * h + 1, r]

    def loaded(k, n):
        if (k, n) in loads:
            loads.pop((k, n)).wait()

    def send_first(k, name, n, step):
        send((k, name, step), first_out.at[k, n], first_in.at[k, n], near[first(k), step])

    def open_half(k, name, n, step, j, h):
        slabs(BLOCK, lambda r: put(first_out, (k, n), r, *pair_of(k, j, h, r)))
        send_first(k, name, n, step)

    def opened(k):
        loaded(k, 0)
        open_half(k, "far", 0, 1, at[first(k), 2], 0)
        open_half(k, "far", 1, -1, at[first(k), 2], 1)

    def opened_near(k):
        loaded(k, 1)
        open_half(k, "near", 2, 1, at[first(k), 1], 1)
        loaded(k, 2)
        open_half(k, "near", 3, -1, at[first(k), -1], 0)

    def relayed(k):
        for h, step in ((0, 1), (1, -1)):
            receive(k, "far", step)

            def add(r):
                a, b = get(first_in, (k, h), r)
                own_a, own_b = pair_of(k, at[first(k), step], h, r)
                put(first_out, (k, 4 + h), r, a + own_a, b + own_b)

            slabs(BLOCK, add)
            send_first(k, "both", 4 + h, step)

    def closed(k):
        loaded(k, 3)
        for h, step in ((0, 1), (1, -1)):
            receive(k, "near", -step)
            receive(k, "both", step)

            def add(r):
                a, b = pair_of(k, at[first(k), 0], h, r)
                near_a, near_b = get(first_in, (k, 3 - h), r)
                both_a, both_b = get(first_in, (k, 4 + h), r)
                total[k, 2 * h, r] = a + near_a + both_a
                total[k, 2 * h + 1, r] = b + near_b + both_b

            slabs(BLOCK, add)
        for n, step in enumerate((2, 1, -1)):
            j = at[second(k), step]
            slabs(HALF, lambda r: put(second_out, (k, n), r, total[k, j, r], total[k, j, lower(r)]))
            send((k, "sum", step), second_out.at[k, n], second_in.at[k, n], near[second(k), step])

    def lower(r):
        return pl.ds(pl.multiple_of(r.start + HALF, SLAB), SLAB)

    def summed(k):
        for step in (1, -1, 2):
            receive(k, "sum", step)

        def add(r):
            top, bottom = total[k, at[second(k), 0], r], total[k, at[second(k), 0], lower(r)]
            for n in range(3):
                a, b = get(second_in, (k, n), r)
                top, bottom = top + a, bottom + b
            fresh[k, r] = top * mean_rate
            fresh[k, lower(r)] = bottom * mean_rate

        slabs(HALF, add)
        mean = fresh[k]
        return SUMS[k](mean * mean)

    def to_cols(buffer, n):
        for k in FAR_FIRST:
            pltpu.make_async_remote_copy(
                src_ref=buffer.at[c],
                dst_ref=buffer.at[c],
                send_sem=norm_send.at[n],
                recv_sem=norm_recv.at[n],
                device_id=(b, across[k]),
                device_id_type=MESH,
            ).start()

    def wait_fifteen(buffer, sem):
        part = buffer.at[pl.ds(0, GROUP - 1)]
        pltpu.make_async_copy(part, part, sem).wait()

    def norms(pair):
        for i, k in enumerate(PAIRS[pair]):
            line = summed(k)
            slope_norms[pair, c, pl.ds(i, 1), pl.ds(0, line.shape[1])] = line
        to_cols(slope_norms.at[pair], 1 + pair)

    def cell(k, j1, j2, h=None):
        t = CHUNKS[k][0]
        return whole.at[(t, j2, j1, rows(k, h)) if first(k) == "x" else (t, j1, j2, rows(k, h))]

    def spread(k, offset, direct):
        a = first(k)
        block = cell(k, at[a, 0], at[second(k), offset])
        for step in (2, 1, -1) if direct else (1, -1):
            send((k, "block", offset, step), block, block, near[a, step])

    def passed(k, offset):
        a = first(k)
        j2 = at[second(k), offset]
        receive(k, "block", offset, 1)
        half = cell(k, at[a, -1], j2, 0)
        send((k, "half", offset, 1), half, half, near[a, 1])
        receive(k, "block", offset, -1)
        half = cell(k, at[a, 1], j2, 1)
        send((k, "half", offset, -1), half, half, near[a, -1])

    def step(pair):
        wait_fifteen(slope_norms.at[pair], norm_recv.at[1 + pair])
        slopes = jnp.sum(slope_norms[pair], axis=0)
        for i, k in enumerate(PAIRS[pair]):
            t, r, n = CHUNKS[k]
            a = second(k)
            ratio = jnp.sqrt(own_sum[t : t + 1, r : r + n] if t < 3 else own_sum[t : t + 1]) * lax.rsqrt(
                slopes[i : i + 1, :n] + 1e-06
            )
            new = weight[t, rows(k)] - learn_rate * (fresh[t, rows(k)] * SPREAD[t](ratio))
            fresh[t, rows(k)] = new
            whole[t, y, x, rows(k)] = new.astype(bf16)
        for k in PAIRS[pair]:
            block = cell(k, at[first(k), 0], at[second(k), 0])
            for s in (2, 1, -1):
                send((k, "line", s), block, block, near[second(k), s])
            spread(k, 0, DIRECT[k])

    def lined(k):
        for s in (1, -1, 2):
            receive(k, "line", s)
            spread(k, -s if s != 2 else 2, DIRECT[k])

    def small_out():
        for copy in small_copies:
            copy.wait()
        for k in range(1, GROUP):
            peer = lax.rem(b + k, GROUP)
            at_lane = pl.multiple_of(peer * BLOCK, BLOCK)
            for i in (0, 1):
                pltpu.make_async_remote_copy(
                    src_ref=small_grad.at[i, :, pl.ds(at_lane, BLOCK)],
                    dst_ref=small_in.at[b, pl.ds(i, 1)],
                    send_sem=small_send.at[0],
                    recv_sem=small_recv.at[0],
                    device_id=(peer, c),
                    device_id_type=MESH,
                ).start()
        own_lane = pl.multiple_of(b * BLOCK, BLOCK)
        small_in[b, pl.ds(0, 1)] = small_grad[0, :, pl.ds(own_lane, BLOCK)]
        small_in[b, pl.ds(1, 1)] = small_grad[1, :, pl.ds(own_lane, BLOCK)]

    def small_step():
        wait_fifteen(small_in, small_recv.at[0])
        small_sum = small_in[0]
        for i in range(1, GROUP):
            small_sum = small_sum + small_in[i]
        small_step = small_weight[...] - learn_rate * (small_sum * mean_rate)
        small_new[...] = small_step
        small_all[b] = small_step
        for k in range(1, GROUP):
            pltpu.make_async_remote_copy(
                src_ref=small_new,
                dst_ref=small_all.at[b],
                send_sem=small_send.at[1],
                recv_sem=small_recv.at[1],
                device_id=(lax.rem(b + k, GROUP), c),
                device_id_type=MESH,
            ).start()

    opened(0)
    opened(1)
    opened_near(0)
    opened_near(1)
    start_loads(1)
    for copy in weight_copies + small_copies:
        copy.start()
    opened(2)
    opened(3)
    opened_near(2)
    opened_near(3)
    for t in range(4):
        weight_copies[t].wait()
        own_norms[c, pl.ds(t, 1)] = SUMS[t](weight[t] * weight[t])
    to_cols(own_norms, 0)
    relayed(0)
    relayed(1)
    relayed(2)
    relayed(3)
    closed(0)
    closed(1)
    closed(2)
    closed(3)
    norms(0)
    norms(1)
    wait_fifteen(own_norms, norm_recv.at[0])
    own_sum = jnp.sum(own_norms[...], axis=0)
    small_out()
    step(0)
    step(1)
    passed(0, 0)
    passed(1, 0)
    lined(0)
    lined(1)
    passed(2, 0)
    passed(3, 0)
    small_step()
    lined(2)
    lined(3)
    for k in (0, 1, 2, 3):
        for offset in (-1, 1, 2):
            passed(k, offset)

    for copy in flight.values():
        copy.wait_recv()
    wait_fifteen(small_all, small_recv.at[1])
    for copy in sent:
        copy.wait_send()
    for n, buffer in ((0, own_norms), (1, slope_norms.at[0]), (2, slope_norms.at[1])):
        wait_fifteen(buffer, norm_send.at[n])
    wait_fifteen(small_in, small_send.at[0])
    wait_fifteen(small_all, small_send.at[1])


def write_out(whole, fresh, small_all, small_own, cq, ck, cv, cm, cn, cb, nq, nk, nv, nm, nn, nb, small, sem):
    copies = []

    def start(src, dst):
        copy = pltpu.make_async_copy(src, dst, sem.at[len(copies)])
        copy.start()
        copies.append(copy)

    for t, out in enumerate((cq, ck, cv)):
        start(whole.at[t], out)
    for j in range(GROUP):
        start(whole.at[3, j // SIDE, j % SIDE], cm.at[:, pl.ds(j * BLOCK, BLOCK)])
    for t, out in enumerate((nq, nk, nv, nm)):
        start(fresh.at[t], out)
    for i, out in enumerate((nn, nb)):
        start(small_own.at[pl.ds(i, 1)], out)
    for i, out in enumerate((cn, cb)):
        small[i] = small_all[:, i].astype(bf16)
        start(small.at[i], out)
    for copy in copies:
        copy.wait()


def per_device(gq, gk, gv, gm, gn, gb, wq, wk, wv, wm, wn, wb):
    blocks = (SIDE, SIDE, BLOCK, BLOCK)
    any_space = pl.BlockSpec(memory_space=pl.ANY)
    in_place = pl.BlockSpec(memory_space=pltpu.VMEM)
    shape = jax.ShapeDtypeStruct
    results = pl.pallas_call(
        kernel,
        out_shape=(
            pltpu.VMEM((4, *blocks), bf16),
            pltpu.VMEM((4, BLOCK, BLOCK), f32),
            pltpu.VMEM((GROUP, 2, BLOCK), f32),
            pltpu.VMEM((2, BLOCK), f32),
        ),
        in_specs=[any_space] * 12,
        out_specs=(in_place,) * 4,
        scratch_shapes=[
            pltpu.VMEM((4, *blocks), f32),
            pltpu.VMEM((4, 6, 3, BLOCK, BLOCK), bf16),
            pltpu.VMEM((4, 6, 3, BLOCK, BLOCK), bf16),
            pltpu.VMEM((4, SIDE, BLOCK, BLOCK), f32),
            pltpu.VMEM((4, 3, 3, HALF, BLOCK), bf16),
            pltpu.VMEM((4, 3, 3, HALF, BLOCK), bf16),
            pltpu.VMEM((4, BLOCK, BLOCK), f32),
            pltpu.VMEM((GROUP, 4, BLOCK), f32),
            pltpu.VMEM((2, GROUP, 2, BLOCK), f32),
            pltpu.VMEM((2, 1, GROUP * BLOCK), f32),
            pltpu.VMEM((GROUP, 2, BLOCK), f32),
            pltpu.VMEM((2, BLOCK), f32),
            pltpu.SemaphoreType.DMA((4, 5)),
            pltpu.SemaphoreType.DMA((120,)),
            pltpu.SemaphoreType.DMA((120,)),
            pltpu.SemaphoreType.DMA((3,)),
            pltpu.SemaphoreType.DMA((3,)),
            pltpu.SemaphoreType.DMA((2,)),
            pltpu.SemaphoreType.DMA((2,)),
            pltpu.SemaphoreType.DMA((4,)),
        ],
        compiler_params=pltpu.CompilerParams(
            collective_id=0, has_side_effects=True, vmem_limit_bytes=24 * 1024 * 1024
        ),
        name="step",
    )(*(
        pltpu.with_memory_space_constraint(a, pltpu.HBM)
        for a in (
            gq.reshape(blocks), gk.reshape(blocks), gv.reshape(blocks), gm[0], gn, gb,
            wq, wk, wv, wm, wn.reshape(1, BLOCK), wb.reshape(1, BLOCK),
        )
    ))
    cq, ck, cv, cm, cn, cb, nq, nk, nv, nm, nn, nb = pl.pallas_call(
        write_out,
        out_shape=(
            shape(blocks, bf16), shape(blocks, bf16), shape(blocks, bf16), shape((BLOCK, GROUP * BLOCK), bf16),
            shape((GROUP, BLOCK), bf16), shape((GROUP, BLOCK), bf16),
            shape((BLOCK, BLOCK), f32), shape((BLOCK, BLOCK), f32), shape((BLOCK, BLOCK), f32), shape((BLOCK, BLOCK), f32),
            shape((1, BLOCK), f32), shape((1, BLOCK), f32),
        ),
        in_specs=[in_place] * 4,
        out_specs=(any_space,) * 12,
        scratch_shapes=[pltpu.VMEM((2, GROUP, BLOCK), bf16), pltpu.SemaphoreType.DMA((32,))],
        compiler_params=pltpu.CompilerParams(vmem_limit_bytes=8 * 1024 * 1024),
        name="write_out",
    )(*(pltpu.with_memory_space_constraint(a, pltpu.VMEM) for a in results))
    whole = (GROUP * BLOCK, BLOCK)
    return (
        cq.reshape(whole), ck.reshape(whole), cv.reshape(whole), cm,
        cn.reshape(-1), cb.reshape(-1),
        nq, nk, nv, nm, nn.reshape(-1), nb.reshape(-1),
    )


def solution(mesh):
    cut = P("batch", "cols")
    in_specs = (
        P("batch", None, "cols"), P("batch", None, "cols"), P("batch", None, "cols"), P("batch", "cols", None),
        P("batch", None), P("batch", None), cut, cut, cut, P("cols", "batch"), P("batch"), P("batch"),
    )
    out_specs = (
        P(None, "cols"), P(None, "cols"), P(None, "cols"), P("cols", None), P(), P(),
        cut, cut, cut, P("cols", "batch"), P("batch"), P("batch"),
    )
    return jax.shard_map(per_device, mesh=mesh, in_specs=in_specs, out_specs=out_specs, check_vma=False)
```

```python
import jax
import jax.numpy as jnp
from jax import lax
from jax.experimental import pallas as pl
from jax.experimental.pallas import tpu as pltpu
from jax.sharding import PartitionSpec as P

learn_rate = 0.4
mean_rate = 0.25
MESH = pl.DeviceIdType.MESH
SIDE = 4
GROUP = 16
BLOCK = 128
HALF = 64
f32 = jnp.float32
bf16 = jnp.bfloat16

FIRST = ("x", "y", "x", "y")
CHUNKS = ((0, 0, 128), (1, 0, 128), (2, 0, 128), (3, 0, 128))
GROUPS = ((0, 1), (2, 3))
ORDER = """
oF1 oF2 oF3 oF0 oN2 oN1 oN3 re2 oN0 re3 re0 re1 cl2 cl3 cl1 cl0 su1 su0 st1 st0 l12 l22 l23 l13
l10 p00 l21 l11 p23 l20 p22 p03 p01 p13 p12 p02 p10 p21 p11 p20
""".split()
FAR_FIRST = (8, 7, 9, 6, 10, 5, 11, 4, 12, 3, 13, 2, 14, 1, 15)


def row_sums(a):
    return jnp.sum(a.T, axis=0, keepdims=True)


def column_sums(a):
    return jnp.sum(a, axis=0, keepdims=True)


def along_rows(line):
    return jnp.broadcast_to(line, (BLOCK, line.shape[1])).T


def along_columns(line):
    return jnp.broadcast_to(line, (BLOCK, BLOCK))


SUMS = (row_sums, row_sums, row_sums, column_sums)
SPREAD = (along_rows, along_rows, along_rows, along_columns)


FIRST_STEPS = 118 * 256.0
SECOND_STEPS = 127 * 256.0
SLAB = 32


def rounded(a):
    head = a.astype(bf16)
    wide = head.astype(f32)
    return head, (a - wide) / jnp.maximum(jnp.abs(wide), 1e-30)


def encode(a, b):
    head_a, left_a = rounded(a)
    head_b, left_b = rounded(b)
    power = jnp.round(left_a * FIRST_STEPS)
    level = jnp.round(left_b * SECOND_STEPS)
    rest = jnp.where(level < 0, level - 128.0, level + 128.0) * jnp.exp2(power)
    return head_a, head_b, rest.astype(bf16)


def decode(head_a, head_b, rest):
    a, b, rest = head_a.astype(f32), head_b.astype(f32), rest.astype(f32)
    size = jnp.abs(rest)
    power = jnp.floor(jnp.log(size) * 1.4426950408889634 + 0.002) - 7.0
    level = size * jnp.exp2(-power) - 128.0
    level = jnp.where(rest < 0, -level, level)
    return a + jnp.abs(a) * (power * (1 / FIRST_STEPS)), b + jnp.abs(b) * (level * (1 / SECOND_STEPS))


def kernel(
    gq, gk, gv, gm, gn, gb, wq, wk, wv, wm, wn, wb,
    whole, fresh, small_all, small_new,
    grad, first_out, first_in, total, second_out, second_in, weight,
    own_norms, slope_norms, small_grad, small_in, small_weight,
    load_sem, send_sem, recv_sem, norm_send, norm_recv, small_send, small_recv, small_load,
):
    b = lax.axis_index("batch")
    c = lax.axis_index("cols")
    y, x = b // SIDE, lax.rem(b, SIDE)
    place = {"y": y, "x": x}
    at = {(a, s): lax.rem(place[a] + s + SIDE, SIDE) for a in "yx" for s in (0, 1, -1, 2)}
    near = {(a, s): ((at[a, s] * SIDE + x) if a == "y" else (y * SIDE + at[a, s]), c) for a in "yx" for s in (1, -1, 2)}
    across = {k: lax.rem(c + k, GROUP) for k in range(1, GROUP)}

    barrier = pltpu.get_barrier_semaphore()
    for a in "yx":
        for s in (1, -1):
            pl.semaphore_signal(barrier, inc=1, device_id=near[a, s], device_id_type=MESH)
    for k in FAR_FIRST:
        pl.semaphore_signal(barrier, inc=1, device_id=(b, across[k]), device_id_type=MESH)

    loads = {}

    def quarter(t, j):
        return grad.at[t, :, j] if FIRST[t] == "x" else grad.at[t, j]

    def start_load(t, n, j):
        g = (gq, gk, gv, gm)[t]
        if t < 3:
            src = g.at[:, j] if FIRST[t] == "x" else g.at[j]
            copy = pltpu.make_async_copy(src, quarter(t, j), load_sem.at[t, n])
            copy.start()
        else:
            for i in range(SIDE):
                at_column = pl.multiple_of((j * SIDE + i) * BLOCK, BLOCK)
                pltpu.make_async_copy(
                    g.at[:, pl.ds(at_column, BLOCK)], grad.at[t, j, i], load_sem.at[t, n]
                ).start()
            copy = pltpu.make_async_copy(quarter(t, j), quarter(t, j), load_sem.at[t, n])
        loads[t, n] = copy

    def start_loads(tensors):
        for n, step in enumerate((2, 1, -1, 0)):
            for t in tensors:
                start_load(t, n, at[FIRST[t], step])

    weight_copies = [pltpu.make_async_copy(w, weight.at[t], load_sem.at[t, 4]) for t, w in enumerate((wq, wk, wv, wm))]
    small_copies = [
        pltpu.make_async_copy(gn, small_grad.at[0], small_load.at[0]),
        pltpu.make_async_copy(gb, small_grad.at[1], small_load.at[1]),
        pltpu.make_async_copy(wn, small_weight.at[pl.ds(0, 1)], small_load.at[2]),
        pltpu.make_async_copy(wb, small_weight.at[pl.ds(1, 1)], small_load.at[3]),
    ]
    needed = []
    for o in ORDER:
        if CHUNKS[int(o[2])][0] not in needed and o[0] == "o":
            needed.append(CHUNKS[int(o[2])][0])
    start_loads(needed[:2])

    pl.semaphore_wait(barrier, 4 + GROUP - 1)

    sent = []
    flight = {}

    def send(key, src, dst, device):
        n = len(sent)
        copy = pltpu.make_async_remote_copy(
            src_ref=src,
            dst_ref=dst,
            send_sem=send_sem.at[n],
            recv_sem=recv_sem.at[n],
            device_id=device,
            device_id_type=MESH,
        )
        copy.start()
        sent.append(copy)
        flight[key] = copy

    def receive(*key):
        flight.pop(key).wait_recv()

    def first(k):
        return FIRST[CHUNKS[k][0]]

    def second(k):
        return "y" if first(k) == "x" else "x"

    def rows(k, h=None):
        _, r, n = CHUNKS[k]
        return pl.ds(r, n) if h is None else pl.ds(r + h * n // 2, n // 2)

    def slabs(start, count, body):
        def one(i, carry):
            body(pl.multiple_of(start + i * SLAB, SLAB))
            return carry

        lax.fori_loop(0, count // SLAB, one, 0)

    def cut(r):
        return pl.ds(r, SLAB)

    def pair_of(k, j, h, r):
        t = CHUNKS[k][0]
        if first(k) == "x":
            return grad[t, 2 * h, j, cut(r)], grad[t, 2 * h + 1, j, cut(r)]
        return grad[t, j, 2 * h, cut(r)], grad[t, j, 2 * h + 1, cut(r)]

    def put(ref, r, values):
        ref[0, cut(r)], ref[1, cut(r)], ref[2, cut(r)] = encode(*values)

    def get(ref, r):
        return decode(ref[0, cut(r)], ref[1, cut(r)], ref[2, cut(r)])

    def loaded(k, n):
        t = CHUNKS[k][0]
        if (t, n) in loads:
            loads.pop((t, n)).wait()

    def send_first(k, name, n, step):
        t = CHUNKS[k][0]
        src, dst = first_out.at[t, n, :, rows(k)], first_in.at[t, n, :, rows(k)]
        send((k, name, step), src, dst, near[first(k), step])

    def open_half(k, name, n, step, j, h):
        t, r0, count = CHUNKS[k]
        slabs(r0, count, lambda r: put(first_out.at[t, n], r, pair_of(k, j, h, r)))
        send_first(k, name, n, step)

    def opened(k):
        loaded(k, 0)
        open_half(k, "far", 0, 1, at[first(k), 2], 0)
        open_half(k, "far", 1, -1, at[first(k), 2], 1)

    def opened_near(k):
        loaded(k, 1)
        open_half(k, "near", 2, 1, at[first(k), 1], 1)
        loaded(k, 2)
        open_half(k, "near", 3, -1, at[first(k), -1], 0)

    def relayed(k):
        t, r0, count = CHUNKS[k]
        for h, step in ((0, 1), (1, -1)):
            receive(k, "far", step)

            def add(r):
                a, b = get(first_in.at[t, h], r)
                own_a, own_b = pair_of(k, at[first(k), step], h, r)
                put(first_out.at[t, 4 + h], r, (a + own_a, b + own_b))

            loaded(k, 1 + h)
            slabs(r0, count, add)
            send_first(k, "both", 4 + h, step)

    def closed(k):
        t, r0, count = CHUNKS[k]
        loaded(k, 3)
        for h, step in ((0, 1), (1, -1)):
            receive(k, "near", -step)
            receive(k, "both", step)

            def add(r):
                a, b = pair_of(k, at[first(k), 0], h, r)
                near_a, near_b = get(first_in.at[t, 3 - h], r)
                both_a, both_b = get(first_in.at[t, 4 + h], r)
                total[t, 2 * h, cut(r)] = a + near_a + both_a
                total[t, 2 * h + 1, cut(r)] = b + near_b + both_b

            slabs(r0, count, add)
        for n, step in enumerate((2, 1, -1)):
            j = at[second(k), step]

            def halves(i):
                r = pl.multiple_of(i + r0 // 2, SLAB)
                low = pl.multiple_of(r + count // 2, SLAB)
                put(second_out.at[t, n], i, (total[t, j, cut(r)], total[t, j, cut(low)]))

            slabs(r0 // 2, count // 2, halves)
            part = pl.ds(r0 // 2, count // 2)
            send((k, "sum", step), second_out.at[t, n, :, part], second_in.at[t, n, :, part], near[second(k), step])

    def summed(k):
        t, r0, count = CHUNKS[k]
        for step in (1, -1, 2):
            receive(k, "sum", step)

        def add(i):
            r = pl.multiple_of(i + r0 // 2, SLAB)
            low = pl.multiple_of(r + count // 2, SLAB)
            top, bottom = total[t, at[second(k), 0], cut(r)], total[t, at[second(k), 0], cut(low)]
            for n in range(3):
                a, b = get(second_in.at[t, n], i)
                top, bottom = top + a, bottom + b
            fresh[t, cut(r)] = top * mean_rate
            fresh[t, cut(low)] = bottom * mean_rate

        slabs(r0 // 2, count // 2, add)
        mean = fresh[t, rows(k)]
        return SUMS[t](mean * mean)

    def to_cols(buffer, n):
        for k in FAR_FIRST:
            pltpu.make_async_remote_copy(
                src_ref=buffer.at[c],
                dst_ref=buffer.at[c],
                send_sem=norm_send.at[n],
                recv_sem=norm_recv.at[n],
                device_id=(b, across[k]),
                device_id_type=MESH,
            ).start()

    def wait_fifteen(buffer, sem):
        part = buffer.at[pl.ds(0, GROUP - 1)]
        pltpu.make_async_copy(part, part, sem).wait()

    def norms(g):
        for i, k in enumerate(GROUPS[g]):
            line = summed(k)
            slope_norms[g, c, pl.ds(i, 1), pl.ds(0, line.shape[1])] = line
        to_cols(slope_norms.at[g], 1 + g)

    def cell(k, j1, j2, h=None):
        t = CHUNKS[k][0]
        return whole.at[(t, j2, j1, rows(k, h)) if first(k) == "x" else (t, j1, j2, rows(k, h))]

    def spread(k, offset):
        a = first(k)
        block = cell(k, at[a, 0], at[second(k), offset])
        for step in (1, -1):
            send((k, "block", offset, step), block, block, near[a, step])

    def passed(k, offset):
        a = first(k)
        j2 = at[second(k), offset]
        receive(k, "block", offset, 1)
        half = cell(k, at[a, -1], j2, 0)
        send((k, "half", offset, 1), half, half, near[a, 1])
        receive(k, "block", offset, -1)
        half = cell(k, at[a, 1], j2, 1)
        send((k, "half", offset, -1), half, half, near[a, -1])

    def step(g):
        wait_fifteen(slope_norms.at[g], norm_recv.at[1 + g])
        slopes = jnp.sum(slope_norms[g], axis=0)
        for i, k in enumerate(GROUPS[g]):
            t, r, n = CHUNKS[k]
            own = jnp.sum(own_norms[...], axis=0)[t : t + 1]
            if t < 3:
                own = own[:, r : r + n]
            ratio = jnp.sqrt(own) * lax.rsqrt(slopes[i : i + 1, : own.shape[1]] + 1e-06)
            new = weight[t, rows(k)] - learn_rate * (fresh[t, rows(k)] * SPREAD[t](ratio))
            fresh[t, rows(k)] = new
            whole[t, y, x, rows(k)] = new.astype(bf16)
            block = cell(k, at[first(k), 0], at[second(k), 0])
            for s in (2, 1, -1):
                send((k, "line", s), block, block, near[second(k), s])
            spread(k, 0)

    def lined(k, *steps):
        for s in steps:
            receive(k, "line", s)
            spread(k, -s if s != 2 else 2)

    def small_out():
        for copy in small_copies:
            copy.wait()
        for k in range(1, GROUP):
            peer = lax.rem(b + k, GROUP)
            at_lane = pl.multiple_of(peer * BLOCK, BLOCK)
            for i in (0, 1):
                pltpu.make_async_remote_copy(
                    src_ref=small_grad.at[i, :, pl.ds(at_lane, BLOCK)],
                    dst_ref=small_in.at[b, pl.ds(i, 1)],
                    send_sem=small_send.at[0],
                    recv_sem=small_recv.at[0],
                    device_id=(peer, c),
                    device_id_type=MESH,
                ).start()
        own_lane = pl.multiple_of(b * BLOCK, BLOCK)
        small_in[b, pl.ds(0, 1)] = small_grad[0, :, pl.ds(own_lane, BLOCK)]
        small_in[b, pl.ds(1, 1)] = small_grad[1, :, pl.ds(own_lane, BLOCK)]

    def small_step():
        wait_fifteen(small_in, small_recv.at[0])
        small_sum = small_in[0]
        for i in range(1, GROUP):
            small_sum = small_sum + small_in[i]
        small_step = small_weight[...] - learn_rate * (small_sum * mean_rate)
        small_new[...] = small_step
        small_all[b] = small_step
        for k in range(1, GROUP):
            pltpu.make_async_remote_copy(
                src_ref=small_new,
                dst_ref=small_all.at[b],
                send_sem=small_send.at[1],
                recv_sem=small_recv.at[1],
                device_id=(lax.rem(b + k, GROUP), c),
                device_id_type=MESH,
            ).start()

    def own_out():
        for t in range(4):
            weight_copies[t].wait()
            own_norms[c, pl.ds(t, 1)] = SUMS[t](weight[t] * weight[t])
        to_cols(own_norms, 0)

    run = {
        "oF": opened,
        "oN": opened_near,
        "re": relayed,
        "cl": closed,
        "su": norms,
        "st": step,
        "p0": lambda k: passed(k, 0),
        "l1": lambda k: lined(k, 1, -1),
        "l2": lambda k: lined(k, 2),
        "p1": lambda k: (passed(k, -1), passed(k, 1)),
        "p2": lambda k: passed(k, 2),
    }
    seen = []
    for o in ORDER:
        if o[:2] == "re" and "re" not in seen:
            own_out()
        if o[:2] == "st" and "st" not in seen:
            small_out()
            wait_fifteen(own_norms, norm_recv.at[0])
        if o[:2] == "p1" and "p1" not in seen:
            small_step()
        run[o[:2]](int(o[2]))
        seen.append(o[:2])
        if len(seen) == 2:
            start_loads(needed[2:])
            for copy in weight_copies + small_copies:
                copy.start()

    for copy in flight.values():
        copy.wait_recv()
    wait_fifteen(small_all, small_recv.at[1])
    for copy in sent:
        copy.wait_send()
    for n, buffer in [(0, own_norms)] + [(1 + g, slope_norms.at[g]) for g in range(len(GROUPS))]:
        wait_fifteen(buffer, norm_send.at[n])
    wait_fifteen(small_in, small_send.at[0])
    wait_fifteen(small_all, small_send.at[1])


def write_out(whole, fresh, small_all, small_own, cq, ck, cv, cm, cn, cb, nq, nk, nv, nm, nn, nb, small, sem):
    copies = []

    def start(src, dst):
        copy = pltpu.make_async_copy(src, dst, sem.at[len(copies)])
        copy.start()
        copies.append(copy)

    for t, out in enumerate((cq, ck, cv)):
        start(whole.at[t], out)
    for j in range(GROUP):
        start(whole.at[3, j // SIDE, j % SIDE], cm.at[:, pl.ds(j * BLOCK, BLOCK)])
    for t, out in enumerate((nq, nk, nv, nm)):
        start(fresh.at[t], out)
    for i, out in enumerate((nn, nb)):
        start(small_own.at[pl.ds(i, 1)], out)
    for i, out in enumerate((cn, cb)):
        small[i] = small_all[:, i].astype(bf16)
        start(small.at[i], out)
    for copy in copies:
        copy.wait()


def per_device(gq, gk, gv, gm, gn, gb, wq, wk, wv, wm, wn, wb):
    blocks = (SIDE, SIDE, BLOCK, BLOCK)
    any_space = pl.BlockSpec(memory_space=pl.ANY)
    in_place = pl.BlockSpec(memory_space=pltpu.VMEM)
    shape = jax.ShapeDtypeStruct
    results = pl.pallas_call(
        kernel,
        out_shape=(
            pltpu.VMEM((4, *blocks), bf16),
            pltpu.VMEM((4, BLOCK, BLOCK), f32),
            pltpu.VMEM((GROUP, 2, BLOCK), f32),
            pltpu.VMEM((2, BLOCK), f32),
        ),
        in_specs=[any_space] * 12,
        out_specs=(in_place,) * 4,
        scratch_shapes=[
            pltpu.VMEM((4, *blocks), f32),
            pltpu.VMEM((4, 6, 3, BLOCK, BLOCK), bf16),
            pltpu.VMEM((4, 6, 3, BLOCK, BLOCK), bf16),
            pltpu.VMEM((4, SIDE, BLOCK, BLOCK), f32),
            pltpu.VMEM((4, 3, 3, HALF, BLOCK), bf16),
            pltpu.VMEM((4, 3, 3, HALF, BLOCK), bf16),
            pltpu.VMEM((4, BLOCK, BLOCK), f32),
            pltpu.VMEM((GROUP, 4, BLOCK), f32),
            pltpu.VMEM((len(GROUPS), GROUP, max(map(len, GROUPS)), BLOCK), f32),
            pltpu.VMEM((2, 1, GROUP * BLOCK), f32),
            pltpu.VMEM((GROUP, 2, BLOCK), f32),
            pltpu.VMEM((2, BLOCK), f32),
            pltpu.SemaphoreType.DMA((4, 5)),
            pltpu.SemaphoreType.DMA((28 * len(CHUNKS),)),
            pltpu.SemaphoreType.DMA((28 * len(CHUNKS),)),
            pltpu.SemaphoreType.DMA((1 + len(GROUPS),)),
            pltpu.SemaphoreType.DMA((1 + len(GROUPS),)),
            pltpu.SemaphoreType.DMA((2,)),
            pltpu.SemaphoreType.DMA((2,)),
            pltpu.SemaphoreType.DMA((4,)),
        ],
        compiler_params=pltpu.CompilerParams(
            collective_id=0, has_side_effects=True, vmem_limit_bytes=24 * 1024 * 1024
        ),
        name="step",
    )(*(
        pltpu.with_memory_space_constraint(a, pltpu.HBM)
        for a in (
            gq.reshape(blocks), gk.reshape(blocks), gv.reshape(blocks), gm[0], gn, gb,
            wq, wk, wv, wm, wn.reshape(1, BLOCK), wb.reshape(1, BLOCK),
        )
    ))
    cq, ck, cv, cm, cn, cb, nq, nk, nv, nm, nn, nb = pl.pallas_call(
        write_out,
        out_shape=(
            shape(blocks, bf16), shape(blocks, bf16), shape(blocks, bf16), shape((BLOCK, GROUP * BLOCK), bf16),
            shape((GROUP, BLOCK), bf16), shape((GROUP, BLOCK), bf16),
            shape((BLOCK, BLOCK), f32), shape((BLOCK, BLOCK), f32), shape((BLOCK, BLOCK), f32), shape((BLOCK, BLOCK), f32),
            shape((1, BLOCK), f32), shape((1, BLOCK), f32),
        ),
        in_specs=[in_place] * 4,
        out_specs=(any_space,) * 12,
        scratch_shapes=[pltpu.VMEM((2, GROUP, BLOCK), bf16), pltpu.SemaphoreType.DMA((32,))],
        compiler_params=pltpu.CompilerParams(vmem_limit_bytes=8 * 1024 * 1024),
        name="write_out",
    )(*(pltpu.with_memory_space_constraint(a, pltpu.VMEM) for a in results))
    whole = (GROUP * BLOCK, BLOCK)
    return (
        cq.reshape(whole), ck.reshape(whole), cv.reshape(whole), cm,
        cn.reshape(-1), cb.reshape(-1),
        nq, nk, nv, nm, nn.reshape(-1), nb.reshape(-1),
    )


def solution(mesh):
    cut = P("batch", "cols")
    in_specs = (
        P("batch", None, "cols"), P("batch", None, "cols"), P("batch", None, "cols"), P("batch", "cols", None),
        P("batch", None), P("batch", None), cut, cut, cut, P("cols", "batch"), P("batch"), P("batch"),
    )
    out_specs = (
        P(None, "cols"), P(None, "cols"), P(None, "cols"), P("cols", None), P(), P(),
        cut, cut, cut, P("cols", "batch"), P("batch"), P("batch"),
    )
    return jax.shard_map(per_device, mesh=mesh, in_specs=in_specs, out_specs=out_specs, check_vma=False)
```

```python
import jax
import jax.numpy as jnp
from jax import lax
from jax.experimental import pallas as pl
from jax.experimental.pallas import tpu as pltpu
from jax.sharding import PartitionSpec as P

learn_rate = 0.4
mean_rate = 0.25
MESH = pl.DeviceIdType.MESH
SIDE = 4
GROUP = 16
BLOCK = 128
HALF = 64
f32 = jnp.float32
bf16 = jnp.bfloat16

FIRST = ("x", "y", "x", "y")
CHUNKS = ((0, 0, 128), (1, 0, 128), (2, 0, 128), (3, 0, 128))
GROUPS = ((0, 1), (2, 3))
ORDER = (
    "oF0", "oF1", "oF3", "oF2", "oN0", "oN1", "re1", "re0", "oN2", "oN3", "re3", "re2", "cl0", "cl1",
    "cl2", "cl3", "su0", "su1", "st0", "st1", "l20", "l10", "l21", "l11", "l12", "l23", "l13", "l22",
    "p03", "p02", "p20", "p21", "p10", "p00", "p11", "p01", "p12", "p23", "p13", "p22",
)
FAR_FIRST = (8, 7, 9, 6, 10, 5, 11, 4, 12, 3, 13, 2, 14, 1, 15)


def row_sums(a):
    return jnp.sum(a.T, axis=0, keepdims=True)


def column_sums(a):
    return jnp.sum(a, axis=0, keepdims=True)


def along_rows(line):
    return jnp.broadcast_to(line, (BLOCK, line.shape[1])).T


def along_columns(line):
    return jnp.broadcast_to(line, (BLOCK, BLOCK))


SUMS = (row_sums, row_sums, row_sums, column_sums)
SPREAD = (along_rows, along_rows, along_rows, along_columns)


FIRST_STEPS = 118 * 256.0
SECOND_STEPS = 127 * 256.0
SLAB = 32


def rounded(a):
    head = a.astype(bf16)
    wide = head.astype(f32)
    return head, (a - wide) / jnp.maximum(jnp.abs(wide), 1e-30)


def encode(a, b):
    head_a, left_a = rounded(a)
    head_b, left_b = rounded(b)
    power = jnp.round(left_a * FIRST_STEPS)
    level = jnp.round(left_b * SECOND_STEPS)
    rest = jnp.where(level < 0, level - 128.0, level + 128.0) * jnp.exp2(power)
    return head_a, head_b, rest.astype(bf16)


def decode(head_a, head_b, rest):
    a, b, rest = head_a.astype(f32), head_b.astype(f32), rest.astype(f32)
    size = jnp.abs(rest)
    power = jnp.floor(jnp.log(size) * 1.4426950408889634 + 0.002) - 7.0
    level = size * jnp.exp2(-power) - 128.0
    level = jnp.where(rest < 0, -level, level)
    return a + jnp.abs(a) * (power * (1 / FIRST_STEPS)), b + jnp.abs(b) * (level * (1 / SECOND_STEPS))


def kernel(
    gq, gk, gv, gm, gn, gb, wq, wk, wv, wm, wn, wb,
    whole, fresh, small_all, small_new,
    grad, first_out, first_in, total, second_out, second_in, weight,
    own_norms, slope_norms, small_grad, small_in, small_weight,
    load_sem, send_sem, recv_sem, norm_send, norm_recv, small_send, small_recv, small_load,
):
    b = lax.axis_index("batch")
    c = lax.axis_index("cols")
    y, x = b // SIDE, lax.rem(b, SIDE)
    place = {"y": y, "x": x}
    at = {(a, s): lax.rem(place[a] + s + SIDE, SIDE) for a in "yx" for s in (0, 1, -1, 2)}
    near = {(a, s): ((at[a, s] * SIDE + x) if a == "y" else (y * SIDE + at[a, s]), c) for a in "yx" for s in (1, -1, 2)}
    across = {k: lax.rem(c + k, GROUP) for k in range(1, GROUP)}

    barrier = pltpu.get_barrier_semaphore()
    for a in "yx":
        for s in (1, -1):
            pl.semaphore_signal(barrier, inc=1, device_id=near[a, s], device_id_type=MESH)
    for k in FAR_FIRST:
        pl.semaphore_signal(barrier, inc=1, device_id=(b, across[k]), device_id_type=MESH)

    loads = {}

    def quarter(t, j):
        return grad.at[t, :, j] if FIRST[t] == "x" else grad.at[t, j]

    def start_load(t, n, j):
        g = (gq, gk, gv, gm)[t]
        if t < 3:
            src = g.at[:, j] if FIRST[t] == "x" else g.at[j]
            copy = pltpu.make_async_copy(src, quarter(t, j), load_sem.at[t, n])
            copy.start()
        else:
            for i in range(SIDE):
                at_column = pl.multiple_of((j * SIDE + i) * BLOCK, BLOCK)
                pltpu.make_async_copy(
                    g.at[:, pl.ds(at_column, BLOCK)], grad.at[t, j, i], load_sem.at[t, n]
                ).start()
            copy = pltpu.make_async_copy(quarter(t, j), quarter(t, j), load_sem.at[t, n])
        loads[t, n] = copy

    def start_loads(tensors):
        for n, step in enumerate((2, 1, -1, 0)):
            for t in tensors:
                start_load(t, n, at[FIRST[t], step])

    weight_copies = [pltpu.make_async_copy(w, weight.at[t], load_sem.at[t, 4]) for t, w in enumerate((wq, wk, wv, wm))]
    small_copies = [
        pltpu.make_async_copy(gn, small_grad.at[0], small_load.at[0]),
        pltpu.make_async_copy(gb, small_grad.at[1], small_load.at[1]),
        pltpu.make_async_copy(wn, small_weight.at[pl.ds(0, 1)], small_load.at[2]),
        pltpu.make_async_copy(wb, small_weight.at[pl.ds(1, 1)], small_load.at[3]),
    ]
    needed = []
    for o in ORDER:
        if CHUNKS[int(o[2])][0] not in needed and o[0] == "o":
            needed.append(CHUNKS[int(o[2])][0])
    start_loads(needed[:2])

    pl.semaphore_wait(barrier, 4 + GROUP - 1)

    sent = []
    flight = {}

    def send(key, src, dst, device):
        n = len(sent)
        copy = pltpu.make_async_remote_copy(
            src_ref=src,
            dst_ref=dst,
            send_sem=send_sem.at[n],
            recv_sem=recv_sem.at[n],
            device_id=device,
            device_id_type=MESH,
        )
        copy.start()
        sent.append(copy)
        flight[key] = copy

    def receive(*key):
        flight.pop(key).wait_recv()

    def first(k):
        return FIRST[CHUNKS[k][0]]

    def second(k):
        return "y" if first(k) == "x" else "x"

    def rows(k, h=None):
        _, r, n = CHUNKS[k]
        return pl.ds(r, n) if h is None else pl.ds(r + h * n // 2, n // 2)

    def slabs(start, count, body):
        def one(i, carry):
            body(pl.multiple_of(start + i * SLAB, SLAB))
            return carry

        lax.fori_loop(0, count // SLAB, one, 0)

    def cut(r):
        return pl.ds(r, SLAB)

    def pair_of(k, j, h, r):
        t = CHUNKS[k][0]
        if first(k) == "x":
            return grad[t, 2 * h, j, cut(r)], grad[t, 2 * h + 1, j, cut(r)]
        return grad[t, j, 2 * h, cut(r)], grad[t, j, 2 * h + 1, cut(r)]

    def put(ref, r, values):
        ref[0, cut(r)], ref[1, cut(r)], ref[2, cut(r)] = encode(*values)

    def get(ref, r):
        return decode(ref[0, cut(r)], ref[1, cut(r)], ref[2, cut(r)])

    def loaded(k, n):
        t = CHUNKS[k][0]
        if (t, n) in loads:
            loads.pop((t, n)).wait()

    def send_first(k, name, n, step):
        t = CHUNKS[k][0]
        src, dst = first_out.at[t, n, :, rows(k)], first_in.at[t, n, :, rows(k)]
        send((k, name, step), src, dst, near[first(k), step])

    def open_half(k, name, n, step, j, h):
        t, r0, count = CHUNKS[k]
        slabs(r0, count, lambda r: put(first_out.at[t, n], r, pair_of(k, j, h, r)))
        send_first(k, name, n, step)

    def opened(k):
        loaded(k, 0)
        open_half(k, "far", 0, 1, at[first(k), 2], 0)
        open_half(k, "far", 1, -1, at[first(k), 2], 1)

    def opened_near(k):
        loaded(k, 1)
        open_half(k, "near", 2, 1, at[first(k), 1], 1)
        loaded(k, 2)
        open_half(k, "near", 3, -1, at[first(k), -1], 0)

    def relayed(k):
        t, r0, count = CHUNKS[k]
        for h, step in ((0, 1), (1, -1)):
            receive(k, "far", step)

            def add(r):
                a, b = get(first_in.at[t, h], r)
                own_a, own_b = pair_of(k, at[first(k), step], h, r)
                put(first_out.at[t, 4 + h], r, (a + own_a, b + own_b))

            loaded(k, 1 + h)
            slabs(r0, count, add)
            send_first(k, "both", 4 + h, step)

    def closed(k):
        t, r0, count = CHUNKS[k]
        loaded(k, 3)
        for h, step in ((0, 1), (1, -1)):
            receive(k, "near", -step)
            receive(k, "both", step)

            def add(r):
                a, b = pair_of(k, at[first(k), 0], h, r)
                near_a, near_b = get(first_in.at[t, 3 - h], r)
                both_a, both_b = get(first_in.at[t, 4 + h], r)
                total[t, 2 * h, cut(r)] = a + near_a + both_a
                total[t, 2 * h + 1, cut(r)] = b + near_b + both_b

            slabs(r0, count, add)
        for n, step in enumerate((2, 1, -1)):
            j = at[second(k), step]

            def halves(i):
                r = pl.multiple_of(i + r0 // 2, SLAB)
                low = pl.multiple_of(r + count // 2, SLAB)
                put(second_out.at[t, n], i, (total[t, j, cut(r)], total[t, j, cut(low)]))

            slabs(r0 // 2, count // 2, halves)
            part = pl.ds(r0 // 2, count // 2)
            send((k, "sum", step), second_out.at[t, n, :, part], second_in.at[t, n, :, part], near[second(k), step])

    def summed(k):
        t, r0, count = CHUNKS[k]
        for step in (1, -1, 2):
            receive(k, "sum", step)

        def add(i):
            r = pl.multiple_of(i + r0 // 2, SLAB)
            low = pl.multiple_of(r + count // 2, SLAB)
            top, bottom = total[t, at[second(k), 0], cut(r)], total[t, at[second(k), 0], cut(low)]
            for n in range(3):
                a, b = get(second_in.at[t, n], i)
                top, bottom = top + a, bottom + b
            fresh[t, cut(r)] = top * mean_rate
            fresh[t, cut(low)] = bottom * mean_rate

        slabs(r0 // 2, count // 2, add)
        mean = fresh[t, rows(k)]
        return SUMS[t](mean * mean)

    def to_cols(buffer, n):
        for k in FAR_FIRST:
            pltpu.make_async_remote_copy(
                src_ref=buffer.at[c],
                dst_ref=buffer.at[c],
                send_sem=norm_send.at[n],
                recv_sem=norm_recv.at[n],
                device_id=(b, across[k]),
                device_id_type=MESH,
            ).start()

    def wait_fifteen(buffer, sem):
        part = buffer.at[pl.ds(0, GROUP - 1)]
        pltpu.make_async_copy(part, part, sem).wait()

    def norms(g):
        for i, k in enumerate(GROUPS[g]):
            line = summed(k)
            slope_norms[g, c, pl.ds(i, 1), pl.ds(0, line.shape[1])] = line
        to_cols(slope_norms.at[g], 1 + g)

    def cell(k, j1, j2, h=None):
        t = CHUNKS[k][0]
        return whole.at[(t, j2, j1, rows(k, h)) if first(k) == "x" else (t, j1, j2, rows(k, h))]

    def spread(k, offset):
        a = first(k)
        block = cell(k, at[a, 0], at[second(k), offset])
        for step in (1, -1):
            send((k, "block", offset, step), block, block, near[a, step])

    def passed(k, offset):
        a = first(k)
        j2 = at[second(k), offset]
        receive(k, "block", offset, 1)
        half = cell(k, at[a, -1], j2, 0)
        send((k, "half", offset, 1), half, half, near[a, 1])
        receive(k, "block", offset, -1)
        half = cell(k, at[a, 1], j2, 1)
        send((k, "half", offset, -1), half, half, near[a, -1])

    def step(g):
        wait_fifteen(slope_norms.at[g], norm_recv.at[1 + g])
        slopes = jnp.sum(slope_norms[g], axis=0)
        for i, k in enumerate(GROUPS[g]):
            t, r, n = CHUNKS[k]
            own = jnp.sum(own_norms[...], axis=0)[t : t + 1]
            if t < 3:
                own = own[:, r : r + n]
            ratio = jnp.sqrt(own) * lax.rsqrt(slopes[i : i + 1, : own.shape[1]] + 1e-06)
            new = weight[t, rows(k)] - learn_rate * (fresh[t, rows(k)] * SPREAD[t](ratio))
            fresh[t, rows(k)] = new
            whole[t, y, x, rows(k)] = new.astype(bf16)
            block = cell(k, at[first(k), 0], at[second(k), 0])
            for s in (2, 1, -1):
                send((k, "line", s), block, block, near[second(k), s])
            spread(k, 0)

    def lined(k, *steps):
        for s in steps:
            receive(k, "line", s)
            spread(k, -s if s != 2 else 2)

    def small_out():
        for copy in small_copies:
            copy.wait()
        for k in range(1, GROUP):
            peer = lax.rem(b + k, GROUP)
            at_lane = pl.multiple_of(peer * BLOCK, BLOCK)
            for i in (0, 1):
                pltpu.make_async_remote_copy(
                    src_ref=small_grad.at[i, :, pl.ds(at_lane, BLOCK)],
                    dst_ref=small_in.at[b, pl.ds(i, 1)],
                    send_sem=small_send.at[0],
                    recv_sem=small_recv.at[0],
                    device_id=(peer, c),
                    device_id_type=MESH,
                ).start()
        own_lane = pl.multiple_of(b * BLOCK, BLOCK)
        small_in[b, pl.ds(0, 1)] = small_grad[0, :, pl.ds(own_lane, BLOCK)]
        small_in[b, pl.ds(1, 1)] = small_grad[1, :, pl.ds(own_lane, BLOCK)]

    def small_step():
        wait_fifteen(small_in, small_recv.at[0])
        small_sum = small_in[0]
        for i in range(1, GROUP):
            small_sum = small_sum + small_in[i]
        small_step = small_weight[...] - learn_rate * (small_sum * mean_rate)
        small_new[...] = small_step
        small_all[b] = small_step
        for k in range(1, GROUP):
            pltpu.make_async_remote_copy(
                src_ref=small_new,
                dst_ref=small_all.at[b],
                send_sem=small_send.at[1],
                recv_sem=small_recv.at[1],
                device_id=(lax.rem(b + k, GROUP), c),
                device_id_type=MESH,
            ).start()

    def own_out():
        for t in range(4):
            weight_copies[t].wait()
            own_norms[c, pl.ds(t, 1)] = SUMS[t](weight[t] * weight[t])
        to_cols(own_norms, 0)

    run = {
        "oF": opened,
        "oN": opened_near,
        "re": relayed,
        "cl": closed,
        "su": norms,
        "st": step,
        "p0": lambda k: passed(k, 0),
        "l1": lambda k: lined(k, 1, -1),
        "l2": lambda k: lined(k, 2),
        "p1": lambda k: (passed(k, -1), passed(k, 1)),
        "p2": lambda k: passed(k, 2),
    }
    seen = []
    for o in ORDER:
        if o[:2] == "re" and "re" not in seen:
            own_out()
        if o[:2] == "st" and "st" not in seen:
            small_out()
            wait_fifteen(own_norms, norm_recv.at[0])
        if o[:2] == "p1" and "p1" not in seen:
            small_step()
        run[o[:2]](int(o[2]))
        seen.append(o[:2])
        if len(seen) == 2:
            start_loads(needed[2:])
            for copy in weight_copies + small_copies:
                copy.start()

    for copy in flight.values():
        copy.wait_recv()
    wait_fifteen(small_all, small_recv.at[1])
    for copy in sent:
        copy.wait_send()
    for n, buffer in [(0, own_norms)] + [(1 + g, slope_norms.at[g]) for g in range(len(GROUPS))]:
        wait_fifteen(buffer, norm_send.at[n])
    wait_fifteen(small_in, small_send.at[0])
    wait_fifteen(small_all, small_send.at[1])


def write_out(whole, fresh, small_all, small_own, cq, ck, cv, cm, cn, cb, nq, nk, nv, nm, nn, nb, small, sem):
    copies = []

    def start(src, dst):
        copy = pltpu.make_async_copy(src, dst, sem.at[len(copies)])
        copy.start()
        copies.append(copy)

    for t, out in enumerate((cq, ck, cv)):
        start(whole.at[t], out)
    for j in range(GROUP):
        start(whole.at[3, j // SIDE, j % SIDE], cm.at[:, pl.ds(j * BLOCK, BLOCK)])
    for t, out in enumerate((nq, nk, nv, nm)):
        start(fresh.at[t], out)
    for i, out in enumerate((nn, nb)):
        start(small_own.at[pl.ds(i, 1)], out)
    for i, out in enumerate((cn, cb)):
        small[i] = small_all[:, i].astype(bf16)
        start(small.at[i], out)
    for copy in copies:
        copy.wait()


def per_device(gq, gk, gv, gm, gn, gb, wq, wk, wv, wm, wn, wb):
    blocks = (SIDE, SIDE, BLOCK, BLOCK)
    any_space = pl.BlockSpec(memory_space=pl.ANY)
    in_place = pl.BlockSpec(memory_space=pltpu.VMEM)
    shape = jax.ShapeDtypeStruct
    results = pl.pallas_call(
        kernel,
        out_shape=(
            pltpu.VMEM((4, *blocks), bf16),
            pltpu.VMEM((4, BLOCK, BLOCK), f32),
            pltpu.VMEM((GROUP, 2, BLOCK), f32),
            pltpu.VMEM((2, BLOCK), f32),
        ),
        in_specs=[any_space] * 12,
        out_specs=(in_place,) * 4,
        scratch_shapes=[
            pltpu.VMEM((4, *blocks), f32),
            pltpu.VMEM((4, 6, 3, BLOCK, BLOCK), bf16),
            pltpu.VMEM((4, 6, 3, BLOCK, BLOCK), bf16),
            pltpu.VMEM((4, SIDE, BLOCK, BLOCK), f32),
            pltpu.VMEM((4, 3, 3, HALF, BLOCK), bf16),
            pltpu.VMEM((4, 3, 3, HALF, BLOCK), bf16),
            pltpu.VMEM((4, BLOCK, BLOCK), f32),
            pltpu.VMEM((GROUP, 4, BLOCK), f32),
            pltpu.VMEM((len(GROUPS), GROUP, max(map(len, GROUPS)), BLOCK), f32),
            pltpu.VMEM((2, 1, GROUP * BLOCK), f32),
            pltpu.VMEM((GROUP, 2, BLOCK), f32),
            pltpu.VMEM((2, BLOCK), f32),
            pltpu.SemaphoreType.DMA((4, 5)),
            pltpu.SemaphoreType.DMA((28 * len(CHUNKS),)),
            pltpu.SemaphoreType.DMA((28 * len(CHUNKS),)),
            pltpu.SemaphoreType.DMA((1 + len(GROUPS),)),
            pltpu.SemaphoreType.DMA((1 + len(GROUPS),)),
            pltpu.SemaphoreType.DMA((2,)),
            pltpu.SemaphoreType.DMA((2,)),
            pltpu.SemaphoreType.DMA((4,)),
        ],
        compiler_params=pltpu.CompilerParams(
            collective_id=0, has_side_effects=True, vmem_limit_bytes=24 * 1024 * 1024
        ),
        name="step",
    )(*(
        pltpu.with_memory_space_constraint(a, pltpu.HBM)
        for a in (
            gq.reshape(blocks), gk.reshape(blocks), gv.reshape(blocks), gm[0], gn, gb,
            wq, wk, wv, wm, wn.reshape(1, BLOCK), wb.reshape(1, BLOCK),
        )
    ))
    cq, ck, cv, cm, cn, cb, nq, nk, nv, nm, nn, nb = pl.pallas_call(
        write_out,
        out_shape=(
            shape(blocks, bf16), shape(blocks, bf16), shape(blocks, bf16), shape((BLOCK, GROUP * BLOCK), bf16),
            shape((GROUP, BLOCK), bf16), shape((GROUP, BLOCK), bf16),
            shape((BLOCK, BLOCK), f32), shape((BLOCK, BLOCK), f32), shape((BLOCK, BLOCK), f32), shape((BLOCK, BLOCK), f32),
            shape((1, BLOCK), f32), shape((1, BLOCK), f32),
        ),
        in_specs=[in_place] * 4,
        out_specs=(any_space,) * 12,
        scratch_shapes=[pltpu.VMEM((2, GROUP, BLOCK), bf16), pltpu.SemaphoreType.DMA((32,))],
        compiler_params=pltpu.CompilerParams(vmem_limit_bytes=8 * 1024 * 1024),
        name="write_out",
    )(*(pltpu.with_memory_space_constraint(a, pltpu.VMEM) for a in results))
    whole = (GROUP * BLOCK, BLOCK)
    return (
        cq.reshape(whole), ck.reshape(whole), cv.reshape(whole), cm,
        cn.reshape(-1), cb.reshape(-1),
        nq, nk, nv, nm, nn.reshape(-1), nb.reshape(-1),
    )


def solution(mesh):
    cut = P("batch", "cols")
    in_specs = (
        P("batch", None, "cols"), P("batch", None, "cols"), P("batch", None, "cols"), P("batch", "cols", None),
        P("batch", None), P("batch", None), cut, cut, cut, P("cols", "batch"), P("batch"), P("batch"),
    )
    out_specs = (
        P(None, "cols"), P(None, "cols"), P(None, "cols"), P("cols", None), P(), P(),
        cut, cut, cut, P("cols", "batch"), P("batch"), P("batch"),
    )
    return jax.shard_map(per_device, mesh=mesh, in_specs=in_specs, out_specs=out_specs, check_vma=False)
```

```python
import jax
import jax.numpy as jnp
from jax import lax
from jax.experimental import pallas as pl
from jax.experimental.pallas import tpu as pltpu
from jax.sharding import PartitionSpec as P

learn_rate = 0.4
mean_rate = 0.25
MESH = pl.DeviceIdType.MESH
SIDE = 4
GROUP = 16
BLOCK = 128
HALF = 64
f32 = jnp.float32
bf16 = jnp.bfloat16

FIRST = ("x", "y", "x", "y")
CHUNKS = ((0, 0, 128), (1, 0, 128), (2, 0, 128), (3, 0, 128))
GROUPS = ((0, 1), (2, 3))
ORDER = (
    "oF0", "oF1", "oF2", "oN0", "oF3", "oN1", "re0", "re1", "oN3", "re2", "oN2", "re3", "cl1", "cl0",
    "cl2", "cl3", "su0", "su1", "st0", "st1", "l10", "l11", "l21", "l20", "l22", "l12", "l23", "l13",
    "p10", "p21", "p03", "p11", "p20", "p22", "p02", "p23", "p00", "p01", "p12", "p13",
)
FAR_FIRST = (8, 7, 9, 6, 10, 5, 11, 4, 12, 3, 13, 2, 14, 1, 15)


def row_sums(a):
    return jnp.sum(a.T, axis=0, keepdims=True)


def column_sums(a):
    return jnp.sum(a, axis=0, keepdims=True)


def along_rows(line):
    return jnp.broadcast_to(line, (BLOCK, line.shape[1])).T


def along_columns(line):
    return jnp.broadcast_to(line, (BLOCK, BLOCK))


SUMS = (row_sums, row_sums, row_sums, column_sums)
SPREAD = (along_rows, along_rows, along_rows, along_columns)


FIRST_STEPS = 118 * 256.0
SECOND_STEPS = 127 * 256.0
SLAB = 64


def rounded(a):
    head = a.astype(bf16)
    wide = head.astype(f32)
    return head, (a - wide) / jnp.maximum(jnp.abs(wide), 1e-30)


def encode(a, b):
    head_a, left_a = rounded(a)
    head_b, left_b = rounded(b)
    power = jnp.round(left_a * FIRST_STEPS)
    level = jnp.round(left_b * SECOND_STEPS)
    rest = jnp.where(level < 0, level - 128.0, level + 128.0) * jnp.exp2(power)
    return head_a, head_b, rest.astype(bf16)


def decode(head_a, head_b, rest):
    a, b, rest = head_a.astype(f32), head_b.astype(f32), rest.astype(f32)
    size = jnp.abs(rest)
    power = jnp.floor(jnp.log(size) * 1.4426950408889634 + 0.002) - 7.0
    level = size * jnp.exp2(-power) - 128.0
    level = jnp.where(rest < 0, -level, level)
    return a + jnp.abs(a) * (power * (1 / FIRST_STEPS)), b + jnp.abs(b) * (level * (1 / SECOND_STEPS))


def kernel(
    gq, gk, gv, gm, gn, gb, wq, wk, wv, wm, wn, wb,
    whole, fresh, small_all, small_new,
    grad, first_out, first_in, total, second_out, second_in, weight,
    own_norms, slope_norms, small_grad, small_in, small_weight,
    load_sem, send_sem, recv_sem, norm_send, norm_recv, small_send, small_recv, small_load,
):
    b = lax.axis_index("batch")
    c = lax.axis_index("cols")
    y, x = b // SIDE, lax.rem(b, SIDE)
    place = {"y": y, "x": x}
    at = {(a, s): lax.rem(place[a] + s + SIDE, SIDE) for a in "yx" for s in (0, 1, -1, 2)}
    near = {(a, s): ((at[a, s] * SIDE + x) if a == "y" else (y * SIDE + at[a, s]), c) for a in "yx" for s in (1, -1, 2)}
    across = {k: lax.rem(c + k, GROUP) for k in range(1, GROUP)}

    barrier = pltpu.get_barrier_semaphore()
    for a in "yx":
        for s in (1, -1):
            pl.semaphore_signal(barrier, inc=1, device_id=near[a, s], device_id_type=MESH)
    for k in FAR_FIRST:
        pl.semaphore_signal(barrier, inc=1, device_id=(b, across[k]), device_id_type=MESH)

    loads = {}

    def quarter(t, j):
        return grad.at[t, :, j] if FIRST[t] == "x" else grad.at[t, j]

    def start_load(t, n, j):
        g = (gq, gk, gv, gm)[t]
        if t < 3:
            src = g.at[:, j] if FIRST[t] == "x" else g.at[j]
            copy = pltpu.make_async_copy(src, quarter(t, j), load_sem.at[t, n])
            copy.start()
        else:
            for i in range(SIDE):
                at_column = pl.multiple_of((j * SIDE + i) * BLOCK, BLOCK)
                pltpu.make_async_copy(
                    g.at[:, pl.ds(at_column, BLOCK)], grad.at[t, j, i], load_sem.at[t, n]
                ).start()
            copy = pltpu.make_async_copy(quarter(t, j), quarter(t, j), load_sem.at[t, n])
        loads[t, n] = copy

    def start_loads(tensors):
        for n, step in enumerate((2, 1, -1, 0)):
            for t in tensors:
                start_load(t, n, at[FIRST[t], step])

    weight_copies = [pltpu.make_async_copy(w, weight.at[t], load_sem.at[t, 4]) for t, w in enumerate((wq, wk, wv, wm))]
    small_copies = [
        pltpu.make_async_copy(gn, small_grad.at[0], small_load.at[0]),
        pltpu.make_async_copy(gb, small_grad.at[1], small_load.at[1]),
        pltpu.make_async_copy(wn, small_weight.at[pl.ds(0, 1)], small_load.at[2]),
        pltpu.make_async_copy(wb, small_weight.at[pl.ds(1, 1)], small_load.at[3]),
    ]
    needed = []
    for o in ORDER:
        if CHUNKS[int(o[2])][0] not in needed and o[0] == "o":
            needed.append(CHUNKS[int(o[2])][0])
    start_loads(needed[:2])

    pl.semaphore_wait(barrier, 4 + GROUP - 1)

    sent = []
    flight = {}

    def send(key, src, dst, device):
        n = len(sent)
        copy = pltpu.make_async_remote_copy(
            src_ref=src,
            dst_ref=dst,
            send_sem=send_sem.at[n],
            recv_sem=recv_sem.at[n],
            device_id=device,
            device_id_type=MESH,
        )
        copy.start()
        sent.append(copy)
        flight[key] = copy

    def receive(*key):
        flight.pop(key).wait_recv()

    def first(k):
        return FIRST[CHUNKS[k][0]]

    def second(k):
        return "y" if first(k) == "x" else "x"

    def rows(k, h=None):
        _, r, n = CHUNKS[k]
        return pl.ds(r, n) if h is None else pl.ds(r + h * n // 2, n // 2)

    def slabs(start, count, body):
        def one(i, carry):
            body(pl.multiple_of(start + i * SLAB, SLAB))
            return carry

        lax.fori_loop(0, count // SLAB, one, 0)

    def cut(r):
        return pl.ds(r, SLAB)

    def pair_of(k, j, h, r):
        t = CHUNKS[k][0]
        if first(k) == "x":
            return grad[t, 2 * h, j, cut(r)], grad[t, 2 * h + 1, j, cut(r)]
        return grad[t, j, 2 * h, cut(r)], grad[t, j, 2 * h + 1, cut(r)]

    def put(ref, r, values):
        ref[0, cut(r)], ref[1, cut(r)], ref[2, cut(r)] = encode(*values)

    def get(ref, r):
        return decode(ref[0, cut(r)], ref[1, cut(r)], ref[2, cut(r)])

    def loaded(k, n):
        t = CHUNKS[k][0]
        if (t, n) in loads:
            loads.pop((t, n)).wait()

    def send_first(k, name, n, step):
        t = CHUNKS[k][0]
        src, dst = first_out.at[t, n, :, rows(k)], first_in.at[t, n, :, rows(k)]
        send((k, name, step), src, dst, near[first(k), step])

    def open_half(k, name, n, step, j, h):
        t, r0, count = CHUNKS[k]
        slabs(r0, count, lambda r: put(first_out.at[t, n], r, pair_of(k, j, h, r)))
        send_first(k, name, n, step)

    def opened(k):
        loaded(k, 0)
        open_half(k, "far", 0, 1, at[first(k), 2], 0)
        open_half(k, "far", 1, -1, at[first(k), 2], 1)

    def opened_near(k):
        loaded(k, 1)
        open_half(k, "near", 2, 1, at[first(k), 1], 1)
        loaded(k, 2)
        open_half(k, "near", 3, -1, at[first(k), -1], 0)

    def relayed(k):
        t, r0, count = CHUNKS[k]
        for h, step in ((0, 1), (1, -1)):
            receive(k, "far", step)

            def add(r):
                a, b = get(first_in.at[t, h], r)
                own_a, own_b = pair_of(k, at[first(k), step], h, r)
                put(first_out.at[t, 4 + h], r, (a + own_a, b + own_b))

            loaded(k, 1 + h)
            slabs(r0, count, add)
            send_first(k, "both", 4 + h, step)

    def closed(k):
        t, r0, count = CHUNKS[k]
        loaded(k, 3)
        for h, step in ((0, 1), (1, -1)):
            receive(k, "near", -step)
            receive(k, "both", step)

            def add(r):
                a, b = pair_of(k, at[first(k), 0], h, r)
                near_a, near_b = get(first_in.at[t, 3 - h], r)
                both_a, both_b = get(first_in.at[t, 4 + h], r)
                total[t, 2 * h, cut(r)] = a + near_a + both_a
                total[t, 2 * h + 1, cut(r)] = b + near_b + both_b

            slabs(r0, count, add)
        for n, step in enumerate((2, 1, -1)):
            j = at[second(k), step]

            def halves(i):
                r = pl.multiple_of(i + r0 // 2, SLAB)
                low = pl.multiple_of(r + count // 2, SLAB)
                put(second_out.at[t, n], i, (total[t, j, cut(r)], total[t, j, cut(low)]))

            slabs(r0 // 2, count // 2, halves)
            part = pl.ds(r0 // 2, count // 2)
            send((k, "sum", step), second_out.at[t, n, :, part], second_in.at[t, n, :, part], near[second(k), step])

    def summed(k):
        t, r0, count = CHUNKS[k]
        for step in (1, -1, 2):
            receive(k, "sum", step)

        def add(i):
            r = pl.multiple_of(i + r0 // 2, SLAB)
            low = pl.multiple_of(r + count // 2, SLAB)
            top, bottom = total[t, at[second(k), 0], cut(r)], total[t, at[second(k), 0], cut(low)]
            for n in range(3):
                a, b = get(second_in.at[t, n], i)
                top, bottom = top + a, bottom + b
            fresh[t, cut(r)] = top * mean_rate
            fresh[t, cut(low)] = bottom * mean_rate

        slabs(r0 // 2, count // 2, add)
        mean = fresh[t, rows(k)]
        return SUMS[t](mean * mean)

    def to_cols(buffer, n):
        for k in FAR_FIRST:
            pltpu.make_async_remote_copy(
                src_ref=buffer.at[c],
                dst_ref=buffer.at[c],
                send_sem=norm_send.at[n],
                recv_sem=norm_recv.at[n],
                device_id=(b, across[k]),
                device_id_type=MESH,
            ).start()

    def wait_fifteen(buffer, sem):
        part = buffer.at[pl.ds(0, GROUP - 1)]
        pltpu.make_async_copy(part, part, sem).wait()

    def norms(g):
        for i, k in enumerate(GROUPS[g]):
            line = summed(k)
            slope_norms[g, c, pl.ds(i, 1), pl.ds(0, line.shape[1])] = line
        to_cols(slope_norms.at[g], 1 + g)

    def cell(k, j1, j2, h=None):
        t = CHUNKS[k][0]
        return whole.at[(t, j2, j1, rows(k, h)) if first(k) == "x" else (t, j1, j2, rows(k, h))]

    def spread(k, offset):
        a = first(k)
        block = cell(k, at[a, 0], at[second(k), offset])
        for step in (1, -1):
            send((k, "block", offset, step), block, block, near[a, step])

    def passed(k, offset):
        a = first(k)
        j2 = at[second(k), offset]
        receive(k, "block", offset, 1)
        half = cell(k, at[a, -1], j2, 0)
        send((k, "half", offset, 1), half, half, near[a, 1])
        receive(k, "block", offset, -1)
        half = cell(k, at[a, 1], j2, 1)
        send((k, "half", offset, -1), half, half, near[a, -1])

    def step(g):
        wait_fifteen(slope_norms.at[g], norm_recv.at[1 + g])
        slopes = jnp.sum(slope_norms[g], axis=0)
        for i, k in enumerate(GROUPS[g]):
            t, r, n = CHUNKS[k]
            own = jnp.sum(own_norms[...], axis=0)[t : t + 1]
            if t < 3:
                own = own[:, r : r + n]
            ratio = jnp.sqrt(own) * lax.rsqrt(slopes[i : i + 1, : own.shape[1]] + 1e-06)
            new = weight[t, rows(k)] - learn_rate * (fresh[t, rows(k)] * SPREAD[t](ratio))
            fresh[t, rows(k)] = new
            whole[t, y, x, rows(k)] = new.astype(bf16)
            block = cell(k, at[first(k), 0], at[second(k), 0])
            for s in (2, 1, -1):
                send((k, "line", s), block, block, near[second(k), s])
            spread(k, 0)

    def lined(k, *steps):
        for s in steps:
            receive(k, "line", s)
            spread(k, -s if s != 2 else 2)

    def small_out():
        for copy in small_copies:
            copy.wait()
        for k in range(1, GROUP):
            peer = lax.rem(b + k, GROUP)
            at_lane = pl.multiple_of(peer * BLOCK, BLOCK)
            for i in (0, 1):
                pltpu.make_async_remote_copy(
                    src_ref=small_grad.at[i, :, pl.ds(at_lane, BLOCK)],
                    dst_ref=small_in.at[b, pl.ds(i, 1)],
                    send_sem=small_send.at[0],
                    recv_sem=small_recv.at[0],
                    device_id=(peer, c),
                    device_id_type=MESH,
                ).start()
        own_lane = pl.multiple_of(b * BLOCK, BLOCK)
        small_in[b, pl.ds(0, 1)] = small_grad[0, :, pl.ds(own_lane, BLOCK)]
        small_in[b, pl.ds(1, 1)] = small_grad[1, :, pl.ds(own_lane, BLOCK)]

    def small_step():
        wait_fifteen(small_in, small_recv.at[0])
        small_sum = small_in[0]
        for i in range(1, GROUP):
            small_sum = small_sum + small_in[i]
        small_step = small_weight[...] - learn_rate * (small_sum * mean_rate)
        small_new[...] = small_step
        small_all[b] = small_step
        for k in range(1, GROUP):
            pltpu.make_async_remote_copy(
                src_ref=small_new,
                dst_ref=small_all.at[b],
                send_sem=small_send.at[1],
                recv_sem=small_recv.at[1],
                device_id=(lax.rem(b + k, GROUP), c),
                device_id_type=MESH,
            ).start()

    def own_out():
        for t in range(4):
            weight_copies[t].wait()
            own_norms[c, pl.ds(t, 1)] = SUMS[t](weight[t] * weight[t])
        to_cols(own_norms, 0)

    run = {
        "oF": opened,
        "oN": opened_near,
        "re": relayed,
        "cl": closed,
        "su": norms,
        "st": step,
        "p0": lambda k: passed(k, 0),
        "l1": lambda k: lined(k, 1, -1),
        "l2": lambda k: lined(k, 2),
        "p1": lambda k: (passed(k, -1), passed(k, 1)),
        "p2": lambda k: passed(k, 2),
    }
    seen = []
    for o in ORDER:
        if o[:2] == "re" and "re" not in seen:
            own_out()
        if o[:2] == "st" and "st" not in seen:
            small_out()
            wait_fifteen(own_norms, norm_recv.at[0])
        if o[:2] == "p1" and "p1" not in seen:
            small_step()
        run[o[:2]](int(o[2]))
        seen.append(o[:2])
        if len(seen) == 2:
            start_loads(needed[2:])
            for copy in weight_copies + small_copies:
                copy.start()

    for copy in flight.values():
        copy.wait_recv()
    wait_fifteen(small_all, small_recv.at[1])
    for copy in sent:
        copy.wait_send()
    for n, buffer in [(0, own_norms)] + [(1 + g, slope_norms.at[g]) for g in range(len(GROUPS))]:
        wait_fifteen(buffer, norm_send.at[n])
    wait_fifteen(small_in, small_send.at[0])
    wait_fifteen(small_all, small_send.at[1])


def write_out(whole, fresh, small_all, small_own, cq, ck, cv, cm, cn, cb, nq, nk, nv, nm, nn, nb, small, sem):
    copies = []

    def start(src, dst):
        copy = pltpu.make_async_copy(src, dst, sem.at[len(copies)])
        copy.start()
        copies.append(copy)

    for t, out in enumerate((cq, ck, cv)):
        start(whole.at[t], out)
    for j in range(GROUP):
        start(whole.at[3, j // SIDE, j % SIDE], cm.at[:, pl.ds(j * BLOCK, BLOCK)])
    for t, out in enumerate((nq, nk, nv, nm)):
        start(fresh.at[t], out)
    for i, out in enumerate((nn, nb)):
        start(small_own.at[pl.ds(i, 1)], out)
    for i, out in enumerate((cn, cb)):
        small[i] = small_all[:, i].astype(bf16)
        start(small.at[i], out)
    for copy in copies:
        copy.wait()


def per_device(gq, gk, gv, gm, gn, gb, wq, wk, wv, wm, wn, wb):
    blocks = (SIDE, SIDE, BLOCK, BLOCK)
    any_space = pl.BlockSpec(memory_space=pl.ANY)
    in_place = pl.BlockSpec(memory_space=pltpu.VMEM)
    shape = jax.ShapeDtypeStruct
    results = pl.pallas_call(
        kernel,
        out_shape=(
            pltpu.VMEM((4, *blocks), bf16),
            pltpu.VMEM((4, BLOCK, BLOCK), f32),
            pltpu.VMEM((GROUP, 2, BLOCK), f32),
            pltpu.VMEM((2, BLOCK), f32),
        ),
        in_specs=[any_space] * 12,
        out_specs=(in_place,) * 4,
        scratch_shapes=[
            pltpu.VMEM((4, *blocks), f32),
            pltpu.VMEM((4, 6, 3, BLOCK, BLOCK), bf16),
            pltpu.VMEM((4, 6, 3, BLOCK, BLOCK), bf16),
            pltpu.VMEM((4, SIDE, BLOCK, BLOCK), f32),
            pltpu.VMEM((4, 3, 3, HALF, BLOCK), bf16),
            pltpu.VMEM((4, 3, 3, HALF, BLOCK), bf16),
            pltpu.VMEM((4, BLOCK, BLOCK), f32),
            pltpu.VMEM((GROUP, 4, BLOCK), f32),
            pltpu.VMEM((len(GROUPS), GROUP, max(map(len, GROUPS)), BLOCK), f32),
            pltpu.VMEM((2, 1, GROUP * BLOCK), f32),
            pltpu.VMEM((GROUP, 2, BLOCK), f32),
            pltpu.VMEM((2, BLOCK), f32),
            pltpu.SemaphoreType.DMA((4, 5)),
            pltpu.SemaphoreType.DMA((28 * len(CHUNKS),)),
            pltpu.SemaphoreType.DMA((28 * len(CHUNKS),)),
            pltpu.SemaphoreType.DMA((1 + len(GROUPS),)),
            pltpu.SemaphoreType.DMA((1 + len(GROUPS),)),
            pltpu.SemaphoreType.DMA((2,)),
            pltpu.SemaphoreType.DMA((2,)),
            pltpu.SemaphoreType.DMA((4,)),
        ],
        compiler_params=pltpu.CompilerParams(
            collective_id=0, has_side_effects=True, vmem_limit_bytes=24 * 1024 * 1024
        ),
        name="step",
    )(*(
        pltpu.with_memory_space_constraint(a, pltpu.HBM)
        for a in (
            gq.reshape(blocks), gk.reshape(blocks), gv.reshape(blocks), gm[0], gn, gb,
            wq, wk, wv, wm, wn.reshape(1, BLOCK), wb.reshape(1, BLOCK),
        )
    ))
    cq, ck, cv, cm, cn, cb, nq, nk, nv, nm, nn, nb = pl.pallas_call(
        write_out,
        out_shape=(
            shape(blocks, bf16), shape(blocks, bf16), shape(blocks, bf16), shape((BLOCK, GROUP * BLOCK), bf16),
            shape((GROUP, BLOCK), bf16), shape((GROUP, BLOCK), bf16),
            shape((BLOCK, BLOCK), f32), shape((BLOCK, BLOCK), f32), shape((BLOCK, BLOCK), f32), shape((BLOCK, BLOCK), f32),
            shape((1, BLOCK), f32), shape((1, BLOCK), f32),
        ),
        in_specs=[in_place] * 4,
        out_specs=(any_space,) * 12,
        scratch_shapes=[pltpu.VMEM((2, GROUP, BLOCK), bf16), pltpu.SemaphoreType.DMA((32,))],
        compiler_params=pltpu.CompilerParams(vmem_limit_bytes=8 * 1024 * 1024),
        name="write_out",
    )(*(pltpu.with_memory_space_constraint(a, pltpu.VMEM) for a in results))
    whole = (GROUP * BLOCK, BLOCK)
    return (
        cq.reshape(whole), ck.reshape(whole), cv.reshape(whole), cm,
        cn.reshape(-1), cb.reshape(-1),
        nq, nk, nv, nm, nn.reshape(-1), nb.reshape(-1),
    )


def solution(mesh):
    cut = P("batch", "cols")
    in_specs = (
        P("batch", None, "cols"), P("batch", None, "cols"), P("batch", None, "cols"), P("batch", "cols", None),
        P("batch", None), P("batch", None), cut, cut, cut, P("cols", "batch"), P("batch"), P("batch"),
    )
    out_specs = (
        P(None, "cols"), P(None, "cols"), P(None, "cols"), P("cols", None), P(), P(),
        cut, cut, cut, P("cols", "batch"), P("batch"), P("batch"),
    )
    return jax.shard_map(per_device, mesh=mesh, in_specs=in_specs, out_specs=out_specs, check_vma=False)
```

```python
import jax
import jax.numpy as jnp
from jax import lax
from jax.experimental import pallas as pl
from jax.experimental.pallas import tpu as pltpu
from jax.sharding import PartitionSpec as P

learn_rate = 0.4
mean_rate = 0.25
MESH = pl.DeviceIdType.MESH
SIDE = 4
GROUP = 16
BLOCK = 128
HALF = 64
f32 = jnp.float32
bf16 = jnp.bfloat16

FIRST = ("x", "y", "x", "y")
CHUNKS = ((0, 0, 128), (1, 0, 128), (2, 0, 128), (3, 0, 128))
GROUPS = ((0, 1), (2, 3))
ORDER = (
    "oF0", "oF1", "oF2", "oN0", "oF3", "oN1", "re0", "re1", "oN3", "re2", "oN2", "re3", "cl1", "cl0",
    "cl2", "cl3", "su0", "su1", "st0", "st1", "l10", "l11", "l21", "l20", "l22", "l12", "l23", "l13",
    "p10", "p21", "p03", "p11", "p20", "p22", "p02", "p23", "p00", "p01", "p12", "p13",
)
FAR_FIRST = (8, 7, 9, 6, 10, 5, 11, 4, 12, 3, 13, 2, 14, 1, 15)


def row_sums(a):
    return jnp.sum(a.T, axis=0, keepdims=True)


def column_sums(a):
    return jnp.sum(a, axis=0, keepdims=True)


def along_rows(line):
    return jnp.broadcast_to(line, (BLOCK, line.shape[1])).T


def along_columns(line):
    return jnp.broadcast_to(line, (BLOCK, BLOCK))


SUMS = (row_sums, row_sums, row_sums, column_sums)
SPREAD = (along_rows, along_rows, along_rows, along_columns)


FIRST_STEPS = 118 * 256.0
SECOND_STEPS = 127 * 256.0
SLAB = 64


def rounded(a):
    head = a.astype(bf16)
    wide = head.astype(f32)
    return head, (a - wide) / jnp.maximum(jnp.abs(wide), 1e-30)


def encode(a, b):
    head_a, left_a = rounded(a)
    head_b, left_b = rounded(b)
    power = jnp.round(left_a * FIRST_STEPS)
    level = jnp.round(left_b * SECOND_STEPS)
    rest = jnp.where(level < 0, level - 128.0, level + 128.0) * jnp.exp2(power)
    return head_a, head_b, rest.astype(bf16)


def decode(head_a, head_b, rest):
    a, b, rest = head_a.astype(f32), head_b.astype(f32), rest.astype(f32)
    size = jnp.abs(rest)
    power = jnp.floor(jnp.log(size) * 1.4426950408889634 + 0.002) - 7.0
    level = size * jnp.exp2(-power) - 128.0
    level = jnp.where(rest < 0, -level, level)
    return a + jnp.abs(a) * (power * (1 / FIRST_STEPS)), b + jnp.abs(b) * (level * (1 / SECOND_STEPS))


def kernel(
    gq, gk, gv, gm, gn, gb, wq, wk, wv, wm, wn, wb,
    whole, fresh, small_all, small_new,
    grad, first_out, first_in, total, second_out, second_in, weight,
    own_norms, slope_norms, small_grad, small_in, small_weight,
    load_sem, send_sem, recv_sem, norm_send, norm_recv, small_send, small_recv, small_load,
):
    b = lax.axis_index("batch")
    c = lax.axis_index("cols")
    y, x = b // SIDE, lax.rem(b, SIDE)
    place = {"y": y, "x": x}
    at = {(a, s): lax.rem(place[a] + s + SIDE, SIDE) for a in "yx" for s in (0, 1, -1, 2)}
    near = {(a, s): ((at[a, s] * SIDE + x) if a == "y" else (y * SIDE + at[a, s]), c) for a in "yx" for s in (1, -1, 2)}
    across = {k: lax.rem(c + k, GROUP) for k in range(1, GROUP)}

    barrier = pltpu.get_barrier_semaphore()
    for a in "yx":
        for s in (1, -1):
            pl.semaphore_signal(barrier, inc=1, device_id=near[a, s], device_id_type=MESH)
    for k in FAR_FIRST:
        pl.semaphore_signal(barrier, inc=1, device_id=(b, across[k]), device_id_type=MESH)

    loads = {}

    def quarter(t, j):
        return grad.at[t, :, j] if FIRST[t] == "x" else grad.at[t, j]

    def start_load(t, n, j):
        g = (gq, gk, gv, gm)[t]
        if t < 3:
            src = g.at[:, j] if FIRST[t] == "x" else g.at[j]
            copy = pltpu.make_async_copy(src, quarter(t, j), load_sem.at[t, n])
            copy.start()
        else:
            for i in range(SIDE):
                at_column = pl.multiple_of((j * SIDE + i) * BLOCK, BLOCK)
                pltpu.make_async_copy(
                    g.at[:, pl.ds(at_column, BLOCK)], grad.at[t, j, i], load_sem.at[t, n]
                ).start()
            copy = pltpu.make_async_copy(quarter(t, j), quarter(t, j), load_sem.at[t, n])
        loads[t, n] = copy

    def start_loads(tensors):
        for n, step in enumerate((2, 1, -1, 0)):
            for t in tensors:
                start_load(t, n, at[FIRST[t], step])

    weight_copies = [pltpu.make_async_copy(w, weight.at[t], load_sem.at[t, 4]) for t, w in enumerate((wq, wk, wv, wm))]
    small_copies = [
        pltpu.make_async_copy(gn, small_grad.at[0], small_load.at[0]),
        pltpu.make_async_copy(gb, small_grad.at[1], small_load.at[1]),
        pltpu.make_async_copy(wn, small_weight.at[pl.ds(0, 1)], small_load.at[2]),
        pltpu.make_async_copy(wb, small_weight.at[pl.ds(1, 1)], small_load.at[3]),
    ]
    needed = []
    for o in ORDER:
        if CHUNKS[int(o[2])][0] not in needed and o[0] == "o":
            needed.append(CHUNKS[int(o[2])][0])
    start_loads(needed[:2])

    pl.semaphore_wait(barrier, 4 + GROUP - 1)

    sent = []
    flight = {}

    def send(key, src, dst, device):
        n = len(sent)
        copy = pltpu.make_async_remote_copy(
            src_ref=src,
            dst_ref=dst,
            send_sem=send_sem.at[n],
            recv_sem=recv_sem.at[n],
            device_id=device,
            device_id_type=MESH,
        )
        copy.start()
        sent.append(copy)
        flight[key] = copy

    def receive(*key):
        flight.pop(key).wait_recv()

    def first(k):
        return FIRST[CHUNKS[k][0]]

    def second(k):
        return "y" if first(k) == "x" else "x"

    def rows(k, h=None):
        _, r, n = CHUNKS[k]
        return pl.ds(r, n) if h is None else pl.ds(r + h * n // 2, n // 2)

    def slabs(start, count, body):
        def one(i, carry):
            body(pl.multiple_of(start + i * SLAB, SLAB))
            return carry

        lax.fori_loop(0, count // SLAB, one, 0, unroll=True)

    def cut(r):
        return pl.ds(r, SLAB)

    def pair_of(k, j, h, r):
        t = CHUNKS[k][0]
        if first(k) == "x":
            return grad[t, 2 * h, j, cut(r)], grad[t, 2 * h + 1, j, cut(r)]
        return grad[t, j, 2 * h, cut(r)], grad[t, j, 2 * h + 1, cut(r)]

    def put(ref, r, values):
        ref[0, cut(r)], ref[1, cut(r)], ref[2, cut(r)] = encode(*values)

    def get(ref, r):
        return decode(ref[0, cut(r)], ref[1, cut(r)], ref[2, cut(r)])

    def loaded(k, n):
        t = CHUNKS[k][0]
        if (t, n) in loads:
            loads.pop((t, n)).wait()

    def send_first(k, name, n, step):
        t = CHUNKS[k][0]
        src, dst = first_out.at[t, n, :, rows(k)], first_in.at[t, n, :, rows(k)]
        send((k, name, step), src, dst, near[first(k), step])

    def open_half(k, name, n, step, j, h):
        t, r0, count = CHUNKS[k]
        slabs(r0, count, lambda r: put(first_out.at[t, n], r, pair_of(k, j, h, r)))
        send_first(k, name, n, step)

    def opened(k):
        loaded(k, 0)
        open_half(k, "far", 0, 1, at[first(k), 2], 0)
        open_half(k, "far", 1, -1, at[first(k), 2], 1)

    def opened_near(k):
        loaded(k, 1)
        open_half(k, "near", 2, 1, at[first(k), 1], 1)
        loaded(k, 2)
        open_half(k, "near", 3, -1, at[first(k), -1], 0)

    def relayed(k):
        t, r0, count = CHUNKS[k]
        for h, step in ((0, 1), (1, -1)):
            receive(k, "far", step)

            def add(r):
                a, b = get(first_in.at[t, h], r)
                own_a, own_b = pair_of(k, at[first(k), step], h, r)
                put(first_out.at[t, 4 + h], r, (a + own_a, b + own_b))

            loaded(k, 1 + h)
            slabs(r0, count, add)
            send_first(k, "both", 4 + h, step)

    def closed(k):
        t, r0, count = CHUNKS[k]
        loaded(k, 3)
        for h, step in ((0, 1), (1, -1)):
            receive(k, "near", -step)
            receive(k, "both", step)

            def add(r):
                a, b = pair_of(k, at[first(k), 0], h, r)
                near_a, near_b = get(first_in.at[t, 3 - h], r)
                both_a, both_b = get(first_in.at[t, 4 + h], r)
                total[t, 2 * h, cut(r)] = a + near_a + both_a
                total[t, 2 * h + 1, cut(r)] = b + near_b + both_b

            slabs(r0, count, add)
        for n, step in enumerate((2, 1, -1)):
            j = at[second(k), step]

            def halves(i):
                r = pl.multiple_of(i + r0 // 2, SLAB)
                low = pl.multiple_of(r + count // 2, SLAB)
                put(second_out.at[t, n], i, (total[t, j, cut(r)], total[t, j, cut(low)]))

            slabs(r0 // 2, count // 2, halves)
            part = pl.ds(r0 // 2, count // 2)
            send((k, "sum", step), second_out.at[t, n, :, part], second_in.at[t, n, :, part], near[second(k), step])

    def summed(k):
        t, r0, count = CHUNKS[k]
        for step in (1, -1, 2):
            receive(k, "sum", step)

        def add(i):
            r = pl.multiple_of(i + r0 // 2, SLAB)
            low = pl.multiple_of(r + count // 2, SLAB)
            top, bottom = total[t, at[second(k), 0], cut(r)], total[t, at[second(k), 0], cut(low)]
            for n in range(3):
                a, b = get(second_in.at[t, n], i)
                top, bottom = top + a, bottom + b
            fresh[t, cut(r)] = top * mean_rate
            fresh[t, cut(low)] = bottom * mean_rate

        slabs(r0 // 2, count // 2, add)
        mean = fresh[t, rows(k)]
        return SUMS[t](mean * mean)

    def to_cols(buffer, n):
        for k in FAR_FIRST:
            pltpu.make_async_remote_copy(
                src_ref=buffer.at[c],
                dst_ref=buffer.at[c],
                send_sem=norm_send.at[n],
                recv_sem=norm_recv.at[n],
                device_id=(b, across[k]),
                device_id_type=MESH,
            ).start()

    def wait_fifteen(buffer, sem):
        part = buffer.at[pl.ds(0, GROUP - 1)]
        pltpu.make_async_copy(part, part, sem).wait()

    def norms(g):
        for i, k in enumerate(GROUPS[g]):
            line = summed(k)
            slope_norms[g, c, pl.ds(i, 1), pl.ds(0, line.shape[1])] = line
        to_cols(slope_norms.at[g], 1 + g)

    def cell(k, j1, j2, h=None):
        t = CHUNKS[k][0]
        return whole.at[(t, j2, j1, rows(k, h)) if first(k) == "x" else (t, j1, j2, rows(k, h))]

    def spread(k, offset):
        a = first(k)
        block = cell(k, at[a, 0], at[second(k), offset])
        for step in (1, -1):
            send((k, "block", offset, step), block, block, near[a, step])

    def passed(k, offset):
        a = first(k)
        j2 = at[second(k), offset]
        receive(k, "block", offset, 1)
        half = cell(k, at[a, -1], j2, 0)
        send((k, "half", offset, 1), half, half, near[a, 1])
        receive(k, "block", offset, -1)
        half = cell(k, at[a, 1], j2, 1)
        send((k, "half", offset, -1), half, half, near[a, -1])

    def step(g):
        wait_fifteen(slope_norms.at[g], norm_recv.at[1 + g])
        slopes = jnp.sum(slope_norms[g], axis=0)
        for i, k in enumerate(GROUPS[g]):
            t, r, n = CHUNKS[k]
            own = jnp.sum(own_norms[...], axis=0)[t : t + 1]
            if t < 3:
                own = own[:, r : r + n]
            ratio = jnp.sqrt(own) * lax.rsqrt(slopes[i : i + 1, : own.shape[1]] + 1e-06)
            new = weight[t, rows(k)] - learn_rate * (fresh[t, rows(k)] * SPREAD[t](ratio))
            fresh[t, rows(k)] = new
            whole[t, y, x, rows(k)] = new.astype(bf16)
            block = cell(k, at[first(k), 0], at[second(k), 0])
            for s in (2, 1, -1):
                send((k, "line", s), block, block, near[second(k), s])
            spread(k, 0)

    def lined(k, *steps):
        for s in steps:
            receive(k, "line", s)
            spread(k, -s if s != 2 else 2)

    def small_out():
        for copy in small_copies:
            copy.wait()
        for k in range(1, GROUP):
            peer = lax.rem(b + k, GROUP)
            at_lane = pl.multiple_of(peer * BLOCK, BLOCK)
            for i in (0, 1):
                pltpu.make_async_remote_copy(
                    src_ref=small_grad.at[i, :, pl.ds(at_lane, BLOCK)],
                    dst_ref=small_in.at[b, pl.ds(i, 1)],
                    send_sem=small_send.at[0],
                    recv_sem=small_recv.at[0],
                    device_id=(peer, c),
                    device_id_type=MESH,
                ).start()
        own_lane = pl.multiple_of(b * BLOCK, BLOCK)
        small_in[b, pl.ds(0, 1)] = small_grad[0, :, pl.ds(own_lane, BLOCK)]
        small_in[b, pl.ds(1, 1)] = small_grad[1, :, pl.ds(own_lane, BLOCK)]

    def small_step():
        wait_fifteen(small_in, small_recv.at[0])
        small_sum = small_in[0]
        for i in range(1, GROUP):
            small_sum = small_sum + small_in[i]
        small_step = small_weight[...] - learn_rate * (small_sum * mean_rate)
        small_new[...] = small_step
        small_all[b] = small_step
        for k in range(1, GROUP):
            pltpu.make_async_remote_copy(
                src_ref=small_new,
                dst_ref=small_all.at[b],
                send_sem=small_send.at[1],
                recv_sem=small_recv.at[1],
                device_id=(lax.rem(b + k, GROUP), c),
                device_id_type=MESH,
            ).start()

    def own_out():
        for t in range(4):
            weight_copies[t].wait()
            own_norms[c, pl.ds(t, 1)] = SUMS[t](weight[t] * weight[t])
        to_cols(own_norms, 0)

    run = {
        "oF": opened,
        "oN": opened_near,
        "re": relayed,
        "cl": closed,
        "su": norms,
        "st": step,
        "p0": lambda k: passed(k, 0),
        "l1": lambda k: lined(k, 1, -1),
        "l2": lambda k: lined(k, 2),
        "p1": lambda k: (passed(k, -1), passed(k, 1)),
        "p2": lambda k: passed(k, 2),
    }
    seen = []
    for o in ORDER:
        if o[:2] == "re" and "re" not in seen:
            own_out()
        if o[:2] == "st" and "st" not in seen:
            small_out()
            wait_fifteen(own_norms, norm_recv.at[0])
        if o[:2] == "p1" and "p1" not in seen:
            small_step()
        run[o[:2]](int(o[2]))
        seen.append(o[:2])
        if len(seen) == 2:
            start_loads(needed[2:])
            for copy in weight_copies + small_copies:
                copy.start()

    for copy in flight.values():
        copy.wait_recv()
    wait_fifteen(small_all, small_recv.at[1])
    for copy in sent:
        copy.wait_send()
    for n, buffer in [(0, own_norms)] + [(1 + g, slope_norms.at[g]) for g in range(len(GROUPS))]:
        wait_fifteen(buffer, norm_send.at[n])
    wait_fifteen(small_in, small_send.at[0])
    wait_fifteen(small_all, small_send.at[1])


def write_out(whole, fresh, small_all, small_own, cq, ck, cv, cm, cn, cb, nq, nk, nv, nm, nn, nb, small, sem):
    copies = []

    def start(src, dst):
        copy = pltpu.make_async_copy(src, dst, sem.at[len(copies)])
        copy.start()
        copies.append(copy)

    for t, out in enumerate((cq, ck, cv)):
        start(whole.at[t], out)
    for j in range(GROUP):
        start(whole.at[3, j // SIDE, j % SIDE], cm.at[:, pl.ds(j * BLOCK, BLOCK)])
    for t, out in enumerate((nq, nk, nv, nm)):
        start(fresh.at[t], out)
    for i, out in enumerate((nn, nb)):
        start(small_own.at[pl.ds(i, 1)], out)
    for i, out in enumerate((cn, cb)):
        small[i] = small_all[:, i].astype(bf16)
        start(small.at[i], out)
    for copy in copies:
        copy.wait()


def per_device(gq, gk, gv, gm, gn, gb, wq, wk, wv, wm, wn, wb):
    blocks = (SIDE, SIDE, BLOCK, BLOCK)
    any_space = pl.BlockSpec(memory_space=pl.ANY)
    in_place = pl.BlockSpec(memory_space=pltpu.VMEM)
    shape = jax.ShapeDtypeStruct
    results = pl.pallas_call(
        kernel,
        out_shape=(
            pltpu.VMEM((4, *blocks), bf16),
            pltpu.VMEM((4, BLOCK, BLOCK), f32),
            pltpu.VMEM((GROUP, 2, BLOCK), f32),
            pltpu.VMEM((2, BLOCK), f32),
        ),
        in_specs=[any_space] * 12,
        out_specs=(in_place,) * 4,
        scratch_shapes=[
            pltpu.VMEM((4, *blocks), f32),
            pltpu.VMEM((4, 6, 3, BLOCK, BLOCK), bf16),
            pltpu.VMEM((4, 6, 3, BLOCK, BLOCK), bf16),
            pltpu.VMEM((4, SIDE, BLOCK, BLOCK), f32),
            pltpu.VMEM((4, 3, 3, HALF, BLOCK), bf16),
            pltpu.VMEM((4, 3, 3, HALF, BLOCK), bf16),
            pltpu.VMEM((4, BLOCK, BLOCK), f32),
            pltpu.VMEM((GROUP, 4, BLOCK), f32),
            pltpu.VMEM((len(GROUPS), GROUP, max(map(len, GROUPS)), BLOCK), f32),
            pltpu.VMEM((2, 1, GROUP * BLOCK), f32),
            pltpu.VMEM((GROUP, 2, BLOCK), f32),
            pltpu.VMEM((2, BLOCK), f32),
            pltpu.SemaphoreType.DMA((4, 5)),
            pltpu.SemaphoreType.DMA((28 * len(CHUNKS),)),
            pltpu.SemaphoreType.DMA((28 * len(CHUNKS),)),
            pltpu.SemaphoreType.DMA((1 + len(GROUPS),)),
            pltpu.SemaphoreType.DMA((1 + len(GROUPS),)),
            pltpu.SemaphoreType.DMA((2,)),
            pltpu.SemaphoreType.DMA((2,)),
            pltpu.SemaphoreType.DMA((4,)),
        ],
        compiler_params=pltpu.CompilerParams(
            collective_id=0, has_side_effects=True, vmem_limit_bytes=24 * 1024 * 1024
        ),
        name="step",
    )(*(
        pltpu.with_memory_space_constraint(a, pltpu.HBM)
        for a in (
            gq.reshape(blocks), gk.reshape(blocks), gv.reshape(blocks), gm[0], gn, gb,
            wq, wk, wv, wm, wn.reshape(1, BLOCK), wb.reshape(1, BLOCK),
        )
    ))
    cq, ck, cv, cm, cn, cb, nq, nk, nv, nm, nn, nb = pl.pallas_call(
        write_out,
        out_shape=(
            shape(blocks, bf16), shape(blocks, bf16), shape(blocks, bf16), shape((BLOCK, GROUP * BLOCK), bf16),
            shape((GROUP, BLOCK), bf16), shape((GROUP, BLOCK), bf16),
            shape((BLOCK, BLOCK), f32), shape((BLOCK, BLOCK), f32), shape((BLOCK, BLOCK), f32), shape((BLOCK, BLOCK), f32),
            shape((1, BLOCK), f32), shape((1, BLOCK), f32),
        ),
        in_specs=[in_place] * 4,
        out_specs=(any_space,) * 12,
        scratch_shapes=[pltpu.VMEM((2, GROUP, BLOCK), bf16), pltpu.SemaphoreType.DMA((32,))],
        compiler_params=pltpu.CompilerParams(vmem_limit_bytes=8 * 1024 * 1024),
        name="write_out",
    )(*(pltpu.with_memory_space_constraint(a, pltpu.VMEM) for a in results))
    whole = (GROUP * BLOCK, BLOCK)
    return (
        cq.reshape(whole), ck.reshape(whole), cv.reshape(whole), cm,
        cn.reshape(-1), cb.reshape(-1),
        nq, nk, nv, nm, nn.reshape(-1), nb.reshape(-1),
    )


def solution(mesh):
    cut = P("batch", "cols")
    in_specs = (
        P("batch", None, "cols"), P("batch", None, "cols"), P("batch", None, "cols"), P("batch", "cols", None),
        P("batch", None), P("batch", None), cut, cut, cut, P("cols", "batch"), P("batch"), P("batch"),
    )
    out_specs = (
        P(None, "cols"), P(None, "cols"), P(None, "cols"), P("cols", None), P(), P(),
        cut, cut, cut, P("cols", "batch"), P("batch"), P("batch"),
    )
    return jax.shard_map(per_device, mesh=mesh, in_specs=in_specs, out_specs=out_specs, check_vma=False)
```
